32 devices in a mesh: row: 16 (over z, y, core), col: 2 (over x).
Axes of the slice: x: 2, y: 2, z: 4, core: 2. Of those that a mesh axis runs over, the one named last changes fastest.
Arguments:
- pair_rep: bfloat16 [2048, 2048, 128], P('row', 'col'), may hold values from -6 to 6
- bias_weight: bfloat16 [128, 12], replicated, may hold values from -0.5 to 0.5
- head_weight: float32 [12], replicated, may hold values from -1 to 1
- queries: float32 [192, 2048], P(None, 'row'), may hold values from -48 to 48, as said below
- key_vectors: float32 [192, 2048], P(None, 'col'), may hold values from -48 to 48, as said below
- values: float32 [192, 2048], P(None, 'col'), may hold values from -6 to 6
- query_points: float32 [3, 48, 2048], P(None, None, 'row'), may hold values from -6 to 6
- key_points: float32 [3, 48, 2048], P(None, None, 'col'), may hold values from -6 to 6
- value_points: float32 [3, 96, 2048], P(None, None, 'col'), may hold values from -6 to 6
- rotations: float32 [3, 3, 2048], replicated, may hold values from -1 to 1, as said below
- translations: float32 [3, 2048], replicated, may hold values from -12 to 12
- residue_count: int32 [1], replicated, may hold values from 1024 to 2048
- grad_output: float32 [192, 2048], P(None, 'row'), may hold values from -6 to 6
- grad_points: float32 [3, 96, 2048], P(None, None, 'row'), may hold values from -6 to 6
- grad_pair: bfloat16 [2048, 12, 128], P('row'), may hold values from -2 to 2
Outputs:
- pair_grad: bfloat16 [2048, 2048, 128], P('row', 'col')
- query_grad: float32 [192, 2048], P(None, ('row', 'col'))
- query_point_grad: float32 [3, 48, 2048], P(None, None, ('row', 'col'))
- query_frame_grad: float32 [3, 4, 2048], P(None, None, ('row', 'col'))
- key_grad: float32 [192, 2048], P(None, ('col', 'row'))
- value_grad: float32 [192, 2048], P(None, ('col', 'row'))
- key_point_grad: float32 [3, 48, 2048], P(None, None, ('col', 'row'))
- value_point_grad: float32 [3, 96, 2048], P(None, None, ('col', 'row'))
- key_frame_grad: float32 [3, 4, 2048], P(None, None, ('col', 'row'))
- bias_weight_grad: float32 [128, 12], replicated
- head_weight_grad: float32 [12], replicated
The draws below stay inside these ranges and needn't reach their ends.
Inputs may be any that keep to these rules, and one draw needn't show every extreme that they name: `queries`: entries of order one, except a few residues whose vectors are much larger. `key_vectors`: entries of order one, except a few residues whose vectors are much larger. `rotations`: each residue's 3 x 3 matrix is a rotation: orthonormal with determinant one.
All inputs are finite; a program needn't handle non-finite values.
Results may differ from the reference program's by a relative error of at most 0.0049.
Values sent between devices are 32-bit elements; how exact they have to be, the bound alone decides.
A program may use at most 256 MiB of HBM per device.

```python
import math
import jax
import jax.numpy as jnp
from jax import lax

N = 2048
H = 12
C = 16
PQ = 4
PV = 8
CZ = 128


def drawn_vectors(key):
    base_key = jax.random.fold_in(key, 11)
    first, second = jax.random.split(base_key, 2)
    query_draw = jnp.clip(jax.random.normal(first, (H * C, N), jnp.float32), -4.0, 4.0)
    key_draw = jnp.clip(jax.random.normal(second, (H * C, N), jnp.float32), -4.0, 4.0)
    return (query_draw, key_draw)


def draw_queries(key, part):
    return drawn_vectors(key)[0]


def draw_key_vectors(key, part):
    return drawn_vectors(key)[1]


def draw_rotations(key, part):
    base_key = jax.random.fold_in(key, 23)
    first, second = jax.random.split(base_key)
    scalar = jax.random.uniform(first, (N,), jnp.float32, 0.5, 1.5)
    vector = jax.random.normal(second, (3, N), jnp.float32)
    length = jnp.sqrt(scalar ** 2 + jnp.sum(vector ** 2, axis=0))
    qw = scalar / length
    qx = vector[0] / length
    qy = vector[1] / length
    qz = vector[2] / length
    first_row = jnp.stack([1 - 2 * (qy * qy + qz * qz), 2 * (qx * qy - qw * qz), 2 * (qx * qz + qw * qy)])
    second_row = jnp.stack([2 * (qx * qy + qw * qz), 1 - 2 * (qx * qx + qz * qz), 2 * (qy * qz - qw * qx)])
    third_row = jnp.stack([2 * (qx * qz - qw * qy), 2 * (qy * qz + qw * qx), 1 - 2 * (qx * qx + qy * qy)])
    return jnp.stack([first_row, second_row, third_row])


def levels(stream_key, dims, shards, least, high):
    factor_of, own = 1.0, jax.random.fold_in(stream_key, 6)
    for position, parts in shards:
        heights = jnp.exp(jax.random.uniform(jax.random.fold_in(own, position), (parts,), jnp.float32, least / len(shards), high / len(shards)))
        factor_of = factor_of * jnp.repeat(heights, dims[position] // parts).reshape([-1 if axis == position else 1 for axis in range(len(dims))])
    return factor_of


def gaussian(own_key, shape, deviation, most, pieces=(), kind=jnp.bfloat16):
    loudness = levels(own_key, shape, pieces, -0.22, 0.18) if pieces else 1.0
    drawn = jax.random.normal(own_key, shape, jnp.float32) * deviation * loudness
    return jnp.minimum(jnp.maximum(drawn, -most), most).astype(kind)


def setup_inputs(seed: int = 0) -> dict:
    key_list = jax.random.split(jax.random.key(seed), 16)
    return {
        "pair_rep": gaussian(key_list[0], (N, N, CZ), 1.0, 6.0, ((0, 16), (1, 2))),
        "bias_weight": gaussian(key_list[1], (CZ, H), CZ ** -0.5, 0.5),
        "head_weight": jnp.clip(jax.random.uniform(key_list[2], (H,), jnp.float32, -1.0, 1.0), -1.0, 1.0),
        "queries": draw_queries(jax.random.fold_in(key_list[15], 71), 0),
        "key_vectors": draw_key_vectors(jax.random.fold_in(key_list[15], 71), 0),
        "values": gaussian(key_list[5], (H * C, N), 1.0, 6.0, ((1, 2),), jnp.float32),
        "query_points": gaussian(key_list[6], (3, H * PQ, N), 1.0, 6.0, ((2, 16),), jnp.float32),
        "key_points": gaussian(key_list[7], (3, H * PQ, N), 1.0, 6.0, ((2, 2),), jnp.float32),
        "value_points": gaussian(key_list[8], (3, H * PV, N), 1.0, 6.0, ((2, 2),), jnp.float32),
        "rotations": draw_rotations(jax.random.fold_in(key_list[15], 71), 0),
        "translations": gaussian(key_list[10], (3, N), 2.0, 12.0, (), jnp.float32),
        "residue_count": jax.random.randint(key_list[11], (1,), N // 2, N + 1).astype(jnp.int32),
        "grad_output": gaussian(key_list[12], (H * C, N), 1.0, 6.0, ((1, 16),), jnp.float32),
        "grad_points": gaussian(key_list[13], (3, H * PV, N), 1.0, 6.0, ((2, 16),), jnp.float32),
        "grad_pair": gaussian(key_list[14], (N, H, CZ), 0.3, 2.0, ((0, 16),)),
    }


HIGHEST = lax.Precision.HIGHEST

def globalize(rotation, offset, local):
    return jnp.einsum('xym,ykm->xkm', rotation, local, precision=HIGHEST) + offset[:, None, :]

def rotate_back(rotation, vector):
    return jnp.einsum('xym,xkm->ykm', rotation, vector, precision=HIGHEST)

def frame_terms(grad_global, local):
    rotation_part = jnp.einsum('xkm,ykm->xym', grad_global, local, precision=HIGHEST)
    return jnp.concatenate([rotation_part, lax.optimization_barrier(jnp.sum(grad_global, axis=1))[:, None, :]], axis=1)

def output_frame_terms(point_out, offset, cotan_local, grad_rotated):
    rotation_part = jnp.einsum('xkm,ykm->xym', point_out - offset[:, None, :], cotan_local, precision=HIGHEST)
    return jnp.concatenate([rotation_part, -lax.optimization_barrier(jnp.sum(grad_rotated, axis=1))[:, None, :]], axis=1)

def reference(pair_rep, bias_weight, head_weight, queries, key_vectors, values, query_points, key_points, value_points, rotations, translations, residue_count, grad_output, grad_points, grad_pair):
    logit_scale = math.sqrt(1.0 / 3.0)
    point_scale = math.sqrt(2.0 / (9.0 * PQ))
    inner_scale = 1.0 / math.sqrt(C)
    distance_coef = 0.5 * logit_scale * point_scale * jax.nn.softplus(head_weight)
    query_global = globalize(rotations, translations, query_points).reshape(3, H, PQ, N)
    key_global = globalize(rotations, translations, key_points).reshape(3, H, PQ, N)
    value_global = globalize(rotations, translations, value_points).reshape(3, H, PV, N)
    grad_global = jnp.einsum('xym,ykm->xkm', rotations, grad_points, precision=HIGHEST)
    grad_heads = grad_global.reshape(3, H, PV, N)
    key_heads = key_vectors.reshape(H, C, N)
    value_heads = values.reshape(H, C, N)
    query_heads = queries.reshape(H, C, N)
    out_heads = grad_output.reshape(H, C, N)
    valid = jnp.arange(N) < residue_count[0]
    pair_weight = bias_weight.astype(jnp.float32)
    block = min(128, N)

    def step(carry, start):
        pair_block = lax.dynamic_slice_in_dim(pair_rep, start, block, 0).astype(jnp.float32)
        cotan_pair = lax.dynamic_slice_in_dim(grad_pair, start, block, 0).astype(jnp.float32)
        query_block = lax.dynamic_slice_in_dim(query_heads, start, block, 2)
        out_block = lax.dynamic_slice_in_dim(out_heads, start, block, 2)
        qglobal_block = lax.dynamic_slice_in_dim(query_global, start, block, 3)
        gglobal_block = lax.dynamic_slice_in_dim(grad_heads, start, block, 3)
        inner = jnp.einsum('hci,hcj->hij', query_block, key_heads, precision=HIGHEST)
        cross = jnp.einsum('xhpi,xhpj->hij', qglobal_block, key_global, precision=HIGHEST)
        distance = lax.optimization_barrier(jnp.sum(qglobal_block ** 2, axis=(0, 2)))[:, :, None] + lax.optimization_barrier(jnp.sum(key_global ** 2, axis=(0, 2)))[:, None, :] - 2.0 * cross
        bias = jnp.einsum('ijc,ch->hij', pair_block, pair_weight, precision=HIGHEST)
        logits = logit_scale * (inner_scale * inner + bias) - distance_coef[:, None, None] * distance
        logits = jnp.where(valid[None, None, :], logits, jnp.float32(-1000000000.0))
        row_peak = lax.optimization_barrier(jnp.max(logits, axis=2, keepdims=True))
        exponent = jnp.exp(logits - row_peak)
        attention = exponent / lax.optimization_barrier(jnp.sum(exponent, axis=2, keepdims=True))
        product = jnp.einsum('hci,hcj->hij', out_block, value_heads, precision=HIGHEST) + jnp.einsum('xhvi,xhvj->hij', gglobal_block, value_global, precision=HIGHEST) + jnp.einsum('ijc,ihc->hij', pair_block, cotan_pair, precision=HIGHEST)
        delta = lax.optimization_barrier(jnp.sum(attention * product, axis=2, keepdims=True))
        logit_grad = attention * (product - delta)
        query_grad = logit_scale * inner_scale * jnp.einsum('hij,hcj->hci', logit_grad, key_heads, precision=HIGHEST)
        row_sum = lax.optimization_barrier(jnp.sum(logit_grad, axis=2))
        qpoint_grad = -2.0 * distance_coef[None, :, None, None] * (qglobal_block * row_sum[None, :, None, :] - jnp.einsum('hij,xhpj->xhpi', logit_grad, key_global, precision=HIGHEST))
        qpoint_flat = qpoint_grad.reshape(3, H * PQ, block)
        point_out = jnp.einsum('hij,xhvj->xhvi', attention, value_global, precision=HIGHEST).reshape(3, H * PV, block)
        rot_block = lax.dynamic_slice_in_dim(rotations, start, block, 2)
        shift_block = lax.dynamic_slice_in_dim(translations, start, block, 1)
        local_block = lax.dynamic_slice_in_dim(query_points, start, block, 2)
        cotan_local = lax.dynamic_slice_in_dim(grad_points, start, block, 2)
        gflat_block = gglobal_block.reshape(3, H * PV, block)
        qlocal_grad = rotate_back(rot_block, qpoint_flat)
        qframe = frame_terms(qpoint_flat, local_block) + output_frame_terms(point_out, shift_block, cotan_local, gflat_block)
        key_part = logit_scale * inner_scale * jnp.einsum('hij,hci->hcj', logit_grad, query_block, precision=HIGHEST)
        value_part = jnp.einsum('hij,hci->hcj', attention, out_block, precision=HIGHEST)
        col_sum = lax.optimization_barrier(jnp.sum(logit_grad, axis=1))
        kpoint_part = 2.0 * distance_coef[None, :, None, None] * (jnp.einsum('hij,xhpi->xhpj', logit_grad, qglobal_block, precision=HIGHEST) - key_global * col_sum[None, :, None, :])
        vpoint_part = jnp.einsum('hij,xhvi->xhvj', attention, gglobal_block, precision=HIGHEST)
        grad_rounded = lax.optimization_barrier(logit_grad.astype(jnp.bfloat16)).astype(jnp.float32)
        attn_rounded = lax.optimization_barrier(attention.astype(jnp.bfloat16)).astype(jnp.float32)
        weight_part = logit_scale * jnp.einsum('ijc,hij->ch', pair_block, grad_rounded, precision=HIGHEST)
        distance_part = lax.optimization_barrier(jnp.sum(logit_grad * distance, axis=(1, 2)))
        pair_grad = (logit_scale * jnp.einsum('hij,ch->ijc', grad_rounded, pair_weight, precision=HIGHEST) + jnp.einsum('hij,ihc->ijc', attn_rounded, cotan_pair, precision=HIGHEST)).astype(jnp.bfloat16)
        new_carry = (carry[0] + key_part, carry[1] + value_part, carry[2] + kpoint_part, carry[3] + vpoint_part, carry[4] + weight_part, carry[5] + distance_part)
        return (new_carry, (pair_grad, query_grad.reshape(H * C, block), qlocal_grad, qframe))
    initial = (jnp.zeros((H, C, N), jnp.float32), jnp.zeros((H, C, N), jnp.float32), jnp.zeros((3, H, PQ, N), jnp.float32), jnp.zeros((3, H, PV, N), jnp.float32), jnp.zeros((CZ, H), jnp.float32), jnp.zeros((H,), jnp.float32))
    starts = jnp.arange(N // block, dtype=jnp.int32) * block
    carry, stacked = lax.scan(step, initial, starts)
    pair_grad = stacked[0].reshape(N, N, CZ)
    query_grad = jnp.transpose(stacked[1], (1, 0, 2)).reshape(H * C, N)
    query_point_grad = jnp.transpose(stacked[2], (1, 2, 0, 3)).reshape(3, H * PQ, N)
    query_frame_grad = jnp.transpose(stacked[3], (1, 2, 0, 3)).reshape(3, 4, N)
    kpoint_flat = carry[2].reshape(3, H * PQ, N)
    vpoint_flat = carry[3].reshape(3, H * PV, N)
    key_point_grad = rotate_back(rotations, kpoint_flat)
    value_point_grad = rotate_back(rotations, vpoint_flat)
    key_frame_grad = frame_terms(kpoint_flat, key_points) + frame_terms(vpoint_flat, value_points)
    head_weight_grad = carry[5] * (-0.5 * logit_scale * point_scale) * jax.nn.sigmoid(head_weight)
    return (pair_grad, query_grad, query_point_grad, query_frame_grad, carry[0].reshape(H * C, N), carry[1].reshape(H * C, N), key_point_grad, value_point_grad, key_frame_grad, carry[4], head_weight_grad)
```

```python
import functools
import math

import jax
import jax.numpy as jnp
from jax import lax
from jax.experimental import pallas as pl
from jax.experimental.pallas import tpu as pltpu
from jax.sharding import PartitionSpec as P

F32 = jnp.float32
BF16 = jnp.bfloat16
PAD = 16
VMEM_LIMIT = 67043328


def dot(a, b, dims):
    return lax.dot_general(a, b, (dims, ((), ())), preferred_element_type=F32)


TN = ((0,), (0,))
NT = ((1,), (1,))
NN = ((1,), (0,))


def split2(x):
    hi = x.astype(BF16)
    return hi, (x - hi.astype(F32)).astype(BF16)


def split3(x):
    hi = x.astype(BF16)
    rest = x - hi.astype(F32)
    mid = rest.astype(BF16)
    return hi, mid, (rest - mid.astype(F32)).astype(BF16)


def merged(stats, own):
    peers = stats.shape[0]
    top = stats[0]
    for c in range(1, peers):
        top = jnp.maximum(top, stats[c])
    total = jnp.zeros_like(top)
    upper = jnp.zeros_like(top)
    for c in range(peers):
        f = jnp.exp(stats[c] - top)
        total = total + pltpu.roll(stats[c], 128 - PAD, 1) * f
        upper = upper + pltpu.roll(stats[c], 128 - 2 * PAD, 1) * f
    return jnp.exp(own - top) / total, upper / total


def flip(place, bit):
    size = 1 << bit
    return place + size * (1 - 2 * ((place // size) % 2))


def toggled(place, bits):
    for bit in bits:
        place = flip(place, bit)
    return place


def subsets(bits):
    found = [()]
    for bit in bits:
        found = found + [s + (bit,) for s in found]
    return found


def remote(src, dst, send, recv, device):
    return pltpu.make_async_remote_copy(
        src_ref=src,
        dst_ref=dst,
        send_sem=send,
        recv_sem=recv,
        device_id=device,
        device_id_type=pl.DeviceIdType.MESH,
    )


class Scatter:
    def __init__(self, me, data, lanes, order, slots, send, recv):
        self.me, self.data, self.lanes, self.order = me, data, lanes, order
        self.slots, self.send, self.recv = slots, send, recv
        self.sent = []

    def plan(self, phase):
        first = sum(1 << (len(self.order) - 1 - p) for p in range(phase))
        return self.order[phase], list(enumerate(subsets(self.order[phase + 1 :]), first))

    def block(self, owner):
        return self.data.at[owner, :, self.lanes]

    def copy(self, phase, slot, bits):
        bit = self.order[phase]
        peer = flip(self.me, bit)
        return remote(
            self.block(toggled(peer, bits)),
            self.slots.at[slot],
            self.send.at[slot],
            self.recv.at[slot],
            {"row": peer},
        )

    def start(self, phase):
        _, blocks = self.plan(phase)
        for slot, bits in blocks:
            copy = self.copy(phase, slot, bits)
            copy.start()
            self.sent.append(copy)

    def finish(self, phase):
        _, blocks = self.plan(phase)
        for slot, bits in blocks:
            self.copy(phase, slot, bits).wait_recv()
            owner = toggled(self.me, bits)
            self.data[owner, :, self.lanes] = (
                self.data[owner, :, self.lanes] + self.slots[slot]
            )

    def drain(self):
        for copy in self.sent:
            copy.wait_send()


def main_kernel(
    shape, limit_ref, pair, bias_w, gpair, qcat, kcat, gcat, vcat, qraw,
    a_out, key_out, query_out, small_out,
    pair_buf, lbase, dbase, rows_buf, stats, merge_buf, key_rows, key_t, slots_a, slots_b,
    query_rows, query_t, qslots, small, small_col, small_row, a_stage,
    pair_sem, a_sem, stat_send, stat_recv, send_a, recv_a, send_b, recv_b, q_send, q_recv,
    col_send, col_recv, row_send, row_recv,
):
    heads, block, scale, nr_dev, nc_dev, nq, nv, vwidth, qsize = shape
    n_rows, cols = pair_buf.shape[0], pair_buf.shape[1]
    blocks = n_rows // block
    me = lax.axis_index("row")
    mc = lax.axis_index("col")
    row_peers = [lax.rem(me + s, nr_dev) for s in range(1, nr_dev)]
    col_peers = [lax.rem(mc + s, nc_dev) for s in range(1, nc_dev)]

    def load(i):
        rows = pl.ds(pl.multiple_of(i * block, block), block)
        return pltpu.make_async_copy(pair.at[rows], pair_buf.at[rows], pair_sem.at[i])

    def start_load(i, carry):
        load(i).start()
        return carry

    lax.fori_loop(0, blocks, start_load, 0)
    barrier = pltpu.get_barrier_semaphore()
    for peer in row_peers:
        pl.semaphore_signal(
            barrier, inc=1, device_id={"row": peer}, device_id_type=pl.DeviceIdType.MESH
        )
    for peer in col_peers:
        pl.semaphore_signal(
            barrier, inc=1, device_id={"col": peer}, device_id_type=pl.DeviceIdType.MESH
        )

    def base(h, carry):
        q0, q1, q2 = split3(qcat[h])
        k0, k1, k2 = split3(kcat[h])
        lbase[h] = dot(
            jnp.concatenate([q0, q0, q1, q0, q2, q1], 0),
            jnp.concatenate([k0, k1, k0, k2, k0, k1], 0),
            TN,
        )
        g0, g1 = split2(gcat[h])
        v0, v1 = split2(vcat[h])
        dbase[h] = dot(
            jnp.concatenate([g0, g0, g1], 0), jnp.concatenate([v0, v1, v0], 0), TN
        )
        return carry

    lax.fori_loop(0, heads, base, 0)
    valid = lax.broadcasted_iota(jnp.int32, (block, cols), 1) < limit_ref[0]
    lane = lax.broadcasted_iota(jnp.int32, (block, 128), 1)

    def forward(i, carry):
        load(i).wait()
        first = pl.multiple_of(i * block, block)
        rows = pl.ds(first, block)
        for r in range(block):
            w = jnp.concatenate([bias_w[...], gpair[first + r]], 0)
            rows_buf[r] = dot(w, pair_buf[first + r], NT)
        packed = jnp.ones((block, 128), F32)
        for h in range(heads):
            logit = lbase[h, rows, :] + scale * rows_buf[:, h, :]
            logit = jnp.where(valid, logit, F32(-1000000000.0))
            peak = jnp.max(logit, axis=1, keepdims=True)
            e = jnp.exp(logit - peak)
            d = dbase[h, rows, :] + rows_buf[:, PAD + h, :]
            lbase[h, rows, :] = e
            dbase[h, rows, :] = d
            packed = jnp.where(lane == h, peak, packed)
            packed = jnp.where(lane == PAD + h, jnp.sum(e, axis=1, keepdims=True), packed)
            packed = jnp.where(
                lane == 2 * PAD + h, jnp.sum(e * d, axis=1, keepdims=True), packed
            )
        stats[0, rows, :] = packed
        return carry

    lax.fori_loop(0, blocks, forward, 0)

    pl.semaphore_wait(barrier, nr_dev + nc_dev - 2)
    sent = []

    def stat_copy(s, peer):
        return remote(
            stats.at[0], stats.at[s], stat_send.at[s], stat_recv.at[s], {"col": peer}
        )

    for s, peer in enumerate(col_peers, 1):
        copy = stat_copy(s, peer)
        copy.start()
        sent.append(copy)
    for s, peer in enumerate(col_peers, 1):
        stat_copy(s, peer).wait_recv()
    factor, delta = merged(stats, stats[0])
    merge_buf[0] = factor
    merge_buf[1] = delta

    lane_of = lax.broadcasted_iota(jnp.int32, (n_rows, 128), 1)
    row_of = lax.broadcasted_iota(jnp.int32, (PAD, 128), 0)
    lane_small = lax.broadcasted_iota(jnp.int32, (PAD, 128), 1)
    small[...] = jnp.zeros_like(small)
    key_rows[...] = jnp.zeros_like(key_rows)
    query_rows[...] = jnp.zeros_like(query_rows)

    def sums(h, carry):
        mine = lane_of == h
        pick = lambda x: jnp.sum(jnp.where(mine, x, 0.0), axis=1, keepdims=True)
        att = lbase[h] * pick(merge_buf[0])
        dl = att * (dbase[h] - pick(merge_buf[1]))
        a0 = att.astype(BF16)
        d0, d1 = split2(dl)
        q = jnp.concatenate(split2(qcat[h]), 0)
        k = jnp.concatenate(split2(kcat[h]), 0)
        g = jnp.concatenate(split2(gcat[h]), 0)
        v = jnp.concatenate(split2(vcat[h]), 0)
        kk = dot(q, d0, NN) + dot(q, d1, NN)
        vv = dot(g, a0, NN)
        half = g.shape[0] // 2
        first = pl.multiple_of(h * (nq + nv), 8)
        key_rows[pl.ds(first, nq), :] = kk[:nq] + kk[nq:]
        key_rows[pl.ds(first + nq, nv), :] = vv[:nv] + vv[half : half + nv]
        qq = dot(k, d0, NT) + dot(k, d1, NT)
        qq = qq[:nq] + qq[nq:]
        oo = dot(v, a0, NT)
        first = pl.multiple_of(h * (nq + nv - vwidth), 8)
        query_rows[pl.ds(first, nq), :] = qq
        query_rows[pl.ds(first + nq, nv - vwidth), :] = (
            oo[vwidth:nv] + oo[half + vwidth : half + nv]
        )
        raw = qraw[h]
        span = qsize - vwidth
        part = raw[span : span + 1] * qq[qsize + 1 : qsize + 2] + qq[qsize : qsize + 1]
        part = part - 2.0 * jnp.sum(raw[:span] * qq[vwidth:qsize], axis=0, keepdims=True)
        part = jnp.sum(part, axis=1, keepdims=True)
        small[...] = small[...] + jnp.where(
            (row_of == heads) & (lane_small == h), part, 0.0
        )
        return carry

    lax.fori_loop(0, heads, sums, 0)

    share = cols // nr_dev
    for t in range(key_t.shape[2] // 128):
        part = slice(128 * t, 128 * t + 128)
        key_t[:, :, part] = key_rows[part, :].T.reshape(nr_dev, share, 128)
    qshare = n_rows // nc_dev
    for t in range(query_t.shape[2] // 128):
        part = slice(128 * t, 128 * t + 128)
        query_t[:, :, part] = query_rows[part, :].T.reshape(nc_dev, qshare, 128)

    bits = list(range(nr_dev.bit_length() - 1))
    swapped = bits[:1] + bits[1:3][::-1] + bits[3:]
    cut = slots_a.shape[2]
    streams = [
        Scatter(me, key_t, pl.ds(0, cut), bits, slots_a, send_a, recv_a),
        Scatter(me, key_t, pl.ds(cut, slots_b.shape[2]), swapped, slots_b, send_b, recv_b),
    ]

    def q_copy(s, peer):
        return remote(
            query_t.at[peer], qslots.at[s], q_send.at[s], q_recv.at[s], {"col": peer}
        )

    for s, peer in enumerate(col_peers):
        copy = q_copy(s, peer)
        copy.start()
        sent.append(copy)
    for stream in streams:
        stream.start(0)

    rows_buf[...] = jnp.zeros_like(rows_buf)

    def a_copy(i):
        rows = pl.ds(pl.multiple_of(i * block, block), block)
        slot = lax.rem(i, 2)
        return pltpu.make_async_copy(a_stage.at[slot], a_out.at[rows], a_sem.at[slot])

    def weights(i, carry):
        first = pl.multiple_of(i * block, block)
        rows = pl.ds(first, block)
        slot = lax.rem(i, 2)

        @pl.when(i >= 2)
        def _():
            a_copy(i - 2).wait()

        factor = merge_buf[0, rows, :]
        delta = merge_buf[1, rows, :]
        for h in range(heads):
            att = lbase[h, rows, :] * factor[:, h : h + 1]
            rows_buf[:, h, :] = att * (dbase[h, rows, :] - delta[:, h : h + 1])
            rows_buf[:, PAD + h, :] = att
        acc = small[...]
        for r in range(block):
            a = rows_buf[r].astype(BF16)
            a_stage[slot, r] = a
            acc = acc + scale * dot(a[:PAD], pair_buf[first + r], NN)
        small[...] = acc
        a_copy(i).start()
        return carry

    early = blocks // 4
    lax.fori_loop(0, early, weights, 0)
    for stream in streams:
        stream.finish(0)
        if len(bits) > 1:
            stream.start(1)
    lax.fori_loop(early, blocks, weights, 0)

    def col_copy(s, peer):
        return remote(
            small, small_col.at[s], col_send.at[s], col_recv.at[s], {"col": peer}
        )

    for s, peer in enumerate(col_peers):
        copy = col_copy(s, peer)
        copy.start()
        sent.append(copy)
    total = query_t[mc]
    for s, peer in enumerate(col_peers):
        q_copy(s, peer).wait_recv()
        total = total + qslots[s]
    query_out[...] = total

    for stream in streams:
        if len(bits) > 1:
            stream.finish(1)
        if len(bits) > 2:
            stream.start(2)

    total = small[...]
    for s, peer in enumerate(col_peers):
        col_copy(s, peer).wait_recv()
        total = total + small_col[s]
    small_row[0] = total

    def row_copy(s, peer):
        return remote(
            small_row.at[0], small_row.at[s], row_send.at[s], row_recv.at[s], {"row": peer}
        )

    for s, peer in enumerate(row_peers, 1):
        copy = row_copy(s, peer)
        copy.start()
        sent.append(copy)
    for phase in range(2, len(bits)):
        for stream in streams:
            stream.finish(phase)
            if phase + 1 < len(bits):
                stream.start(phase + 1)
    key_out[...] = key_t[me]
    total = small_row[0]
    for s, peer in enumerate(row_peers, 1):
        row_copy(s, peer).wait_recv()
        total = total + small_row[s]
    small_out[...] = total
    for copy in sent:
        copy.wait_send()
    for stream in streams:
        stream.drain()
    for i in range(max(blocks - 2, 0), blocks):
        a_copy(i).wait()


def pair_kernel(block, a_in, scaled, gpair, pg_out):
    w_hi, w_lo = split2(scaled[...])
    for r in range(block):
        a = a_in[r]
        lhs = jnp.concatenate([a, a[:PAD]], 0)
        rhs = jnp.concatenate([w_hi, gpair[r], w_lo], 0)
        pg_out[r] = dot(lhs, rhs, TN).astype(BF16)


def turn(rotation, local):
    return jnp.sum(rotation[:, :, None, :] * local[None], axis=1)


def turn_back(rotation, vector):
    return jnp.sum(rotation[:, :, None, :] * vector[:, None], axis=0)


def frame_terms(grad_global, local):
    rotation_part = jnp.sum(grad_global[:, None] * local[None], axis=2)
    return jnp.concatenate([rotation_part, jnp.sum(grad_global, axis=1)[:, None, :]], axis=1)


def by_head(x, heads):
    points = x.shape[1] // heads
    return x.reshape(3, heads, points, -1).transpose(1, 0, 2, 3).reshape(heads, 3 * points, -1)


def by_axis(x):
    heads, rows, m = x.shape
    return x.reshape(heads, 3, rows // 3, m).transpose(1, 0, 2, 3).reshape(3, heads * rows // 3, m)


def pad_rows(x, rows):
    return jnp.pad(x, ((0, 0), (0, rows - x.shape[1]), (0, 0)))


def per_device(
    pair_rep, bias_weight, head_weight, queries, key_vectors, values, query_points, key_points,
    value_points, rotations, translations, residue_count, grad_output, grad_points, grad_pair,
):
    channels, heads = bias_weight.shape
    width = queries.shape[0] // heads
    qpoints = query_points.shape[1] // heads
    vpoints = value_points.shape[1] // heads
    n_rows = queries.shape[1]
    n_cols = key_vectors.shape[1]
    logit_scale = math.sqrt(1.0 / 3.0)
    point_scale = math.sqrt(2.0 / (9.0 * qpoints))
    inner_scale = 1.0 / math.sqrt(width)
    coef = 0.5 * logit_scale * point_scale * jax.nn.softplus(head_weight)
    row_start = lax.axis_index("row") * n_rows
    col_start = lax.axis_index("col") * n_cols
    rot_rows = lax.dynamic_slice_in_dim(rotations, row_start, n_rows, 2)
    shift_rows = lax.dynamic_slice_in_dim(translations, row_start, n_rows, 1)
    rot_cols = lax.dynamic_slice_in_dim(rotations, col_start, n_cols, 2)
    shift_cols = lax.dynamic_slice_in_dim(translations, col_start, n_cols, 1)
    qg = by_head(turn(rot_rows, query_points) + shift_rows[:, None, :], heads)
    kg = by_head(turn(rot_cols, key_points) + shift_cols[:, None, :], heads)
    vg = by_head(turn(rot_cols, value_points) + shift_cols[:, None, :], heads)
    grad_flat = turn(rot_rows, grad_points)
    gg = by_head(grad_flat, heads)
    q = queries.reshape(heads, width, n_rows)
    k = key_vectors.reshape(heads, width, n_cols)
    qsize = width + 3 * qpoints
    nq = -(-(qsize + 2) // 16) * 16
    nv = width + 3 * vpoints
    nvp = -(-nv // 16) * 16
    c3 = coef[:, None, None]
    q_square = jnp.sum(qg * qg, axis=1, keepdims=True)
    k_square = jnp.sum(kg * kg, axis=1, keepdims=True)
    qcat = pad_rows(
        jnp.concatenate(
            [
                logit_scale * inner_scale * q,
                2.0 * c3 * qg,
                jnp.broadcast_to(-c3, (heads, 1, n_rows)),
                -c3 * q_square,
            ],
            axis=1,
        ),
        nq,
    )
    kcat = pad_rows(
        jnp.concatenate([k, kg, k_square, jnp.ones((heads, 1, n_cols), F32)], axis=1), nq
    )
    gcat = pad_rows(
        jnp.concatenate([grad_output.reshape(heads, width, n_rows), gg], axis=1), nvp
    )
    vcat = pad_rows(jnp.concatenate([values.reshape(heads, width, n_cols), vg], axis=1), nvp)
    w_t = jnp.pad(bias_weight.T, ((0, PAD - heads), (0, 0)))
    scaled = logit_scale * w_t.astype(F32)
    gpair = pad_rows(grad_pair, PAD)
    limit = residue_count - col_start

    block = 8
    rows_dev = lax.axis_size("row")
    cols_dev = lax.axis_size("col")
    qraw = pad_rows(jnp.concatenate([qg, q_square], axis=1), PAD)
    nk = nq + nv
    nr = nq + nv - width
    key_lanes = -(-heads * nk // 128) * 128
    query_lanes = -(-heads * nr // 128) * 128
    cut = -(-key_lanes // 256) * 128
    kshare = n_cols // rows_dev
    qshare = n_rows // cols_dev
    vmem = pl.BlockSpec(memory_space=pltpu.VMEM)
    anywhere = pl.BlockSpec(memory_space=pl.ANY)
    sems = lambda count: pltpu.SemaphoreType.DMA((max(count, 1),))
    a_all, key_part, query_part, small = pl.pallas_call(
        functools.partial(
            main_kernel,
            (heads, block, logit_scale, rows_dev, cols_dev, nq, nv, width, qsize),
        ),
        in_specs=[pl.BlockSpec(memory_space=pltpu.SMEM), anywhere] + [vmem] * 7,
        out_specs=[anywhere, vmem, vmem, vmem],
        out_shape=[
            jax.ShapeDtypeStruct((n_rows, 2 * PAD, n_cols), BF16),
            jax.ShapeDtypeStruct((kshare, key_lanes), F32),
            jax.ShapeDtypeStruct((qshare, query_lanes), F32),
            jax.ShapeDtypeStruct((PAD, channels), F32),
        ],
        scratch_shapes=[
            pltpu.VMEM((n_rows, n_cols, channels), BF16),
            pltpu.VMEM((heads, n_rows, n_cols), F32),
            pltpu.VMEM((heads, n_rows, n_cols), F32),
            pltpu.VMEM((block, 2 * PAD, n_cols), F32),
            pltpu.VMEM((cols_dev, n_rows, 128), F32),
            pltpu.VMEM((2, n_rows, 128), F32),
            pltpu.VMEM((key_lanes, n_cols), F32),
            pltpu.VMEM((rows_dev, kshare, key_lanes), F32),
            pltpu.VMEM((rows_dev - 1, kshare, cut), F32),
            pltpu.VMEM((rows_dev - 1, kshare, key_lanes - cut), F32),
            pltpu.VMEM((query_lanes, n_rows), F32),
            pltpu.VMEM((cols_dev, qshare, query_lanes), F32),
            pltpu.VMEM((max(cols_dev - 1, 1), qshare, query_lanes), F32),
            pltpu.VMEM((PAD, channels), F32),
            pltpu.VMEM((max(cols_dev - 1, 1), PAD, channels), F32),
            pltpu.VMEM((rows_dev, PAD, channels), F32),
            pltpu.VMEM((2, block, 2 * PAD, n_cols), BF16),
            sems(n_rows // block),
            sems(2),
            sems(cols_dev),
            sems(cols_dev),
            sems(rows_dev - 1),
            sems(rows_dev - 1),
            sems(rows_dev - 1),
            sems(rows_dev - 1),
            sems(cols_dev - 1),
            sems(cols_dev - 1),
            sems(cols_dev - 1),
            sems(cols_dev - 1),
            sems(rows_dev),
            sems(rows_dev),
        ],
        compiler_params=pltpu.CompilerParams(
            collective_id=0, has_side_effects=True, vmem_limit_bytes=VMEM_LIMIT
        ),
    )(limit, pair_rep, w_t, gpair, qcat, kcat, gcat, vcat, qraw)

    out_block = 8
    pair_grad = pl.pallas_call(
        functools.partial(pair_kernel, out_block),
        grid=(n_rows // out_block,),
        in_specs=[
            pl.BlockSpec((out_block, 2 * PAD, n_cols), lambda i: (i, 0, 0)),
            pl.BlockSpec((PAD, channels), lambda i: (0, 0)),
            pl.BlockSpec((out_block, PAD, channels), lambda i: (i, 0, 0)),
        ],
        out_specs=pl.BlockSpec((out_block, n_cols, channels), lambda i: (i, 0, 0)),
        out_shape=jax.ShapeDtypeStruct(pair_rep.shape, BF16),
        compiler_params=pltpu.CompilerParams(dimension_semantics=("arbitrary",)),
    )(a_all, scaled, gpair)

    key_sum = key_part.T[: heads * nk].reshape(heads, nk, kshare)
    query_sum = query_part.T[: heads * nr].reshape(heads, nr, qshare)
    weight_total = small[:heads].T
    head_weight_grad = (
        small[heads, :heads] * (-0.5 * logit_scale * point_scale) * jax.nn.sigmoid(head_weight)
    )

    share = query_sum.shape[2]
    start = lax.axis_index("col") * share
    own_rows = lambda x: lax.dynamic_slice_in_dim(x, start, share, x.ndim - 1)
    rot_own = own_rows(rot_rows)
    shift_own = own_rows(shift_rows)
    query_grad = (logit_scale * inner_scale * query_sum[:, :width]).reshape(heads * width, share)
    dqg = by_axis(
        -2.0 * c3 * (own_rows(qg) * query_sum[:, qsize + 1][:, None] - query_sum[:, width:qsize])
    )
    point_out = by_axis(query_sum[:, nq:])
    query_point_grad = turn_back(rot_own, dqg)
    cotan_own = own_rows(grad_points)
    out_part = jnp.sum((point_out - shift_own[:, None, :])[:, None] * cotan_own[None], axis=2)
    out_part = jnp.concatenate(
        [out_part, -jnp.sum(own_rows(grad_flat), axis=1)[:, None, :]], axis=1
    )
    query_frame_grad = frame_terms(dqg, own_rows(query_points)) + out_part

    kshare = key_sum.shape[2]
    kstart = lax.axis_index("row") * kshare
    own_cols = lambda x: lax.dynamic_slice_in_dim(x, kstart, kshare, x.ndim - 1)
    rot_keys = own_cols(rot_cols)
    key_grad = key_sum[:, :width].reshape(heads * width, kshare)
    value_grad = key_sum[:, nq : nq + width].reshape(heads * width, kshare)
    dkg = by_axis(
        key_sum[:, width:qsize] + 2.0 * own_cols(kg) * key_sum[:, qsize][:, None]
    )
    dvg = by_axis(key_sum[:, nq + width :])
    key_point_grad = turn_back(rot_keys, dkg)
    value_point_grad = turn_back(rot_keys, dvg)
    key_frame_grad = frame_terms(dkg, own_cols(key_points)) + frame_terms(
        dvg, own_cols(value_points)
    )
    return (
        pair_grad, query_grad, query_point_grad, query_frame_grad, key_grad, value_grad,
        key_point_grad, value_point_grad, key_frame_grad, weight_total, head_weight_grad,
    )


def solution(mesh):
    return jax.shard_map(
        per_device,
        mesh=mesh,
        in_specs=(
            P("row", "col", None),
            P(),
            P(),
            P(None, "row"),
            P(None, "col"),
            P(None, "col"),
            P(None, None, "row"),
            P(None, None, "col"),
            P(None, None, "col"),
            P(),
            P(),
            P(),
            P(None, "row"),
            P(None, None, "row"),
            P("row", None, None),
        ),
        out_specs=(
            P("row", "col", None),
            P(None, ("row", "col")),
            P(None, None, ("row", "col")),
            P(None, None, ("row", "col")),
            P(None, ("col", "row")),
            P(None, ("col", "row")),
            P(None, None, ("col", "row")),
            P(None, None, ("col", "row")),
            P(None, None, ("col", "row")),
            P(),
            P(),
        ),
        check_vma=False,
    )
```

```python
import functools
import math

import jax
import jax.numpy as jnp
from jax import lax
from jax.experimental import pallas as pl
from jax.experimental.pallas import tpu as pltpu
from jax.sharding import PartitionSpec as P

F32 = jnp.float32
BF16 = jnp.bfloat16
PAD = 16
VMEM_LIMIT = 67043328


def dot(a, b, dims):
    return lax.dot_general(a, b, (dims, ((), ())), preferred_element_type=F32)


TN = ((0,), (0,))
NT = ((1,), (1,))
NN = ((1,), (0,))


def split2(x):
    hi = x.astype(BF16)
    return hi, (x - hi.astype(F32)).astype(BF16)


def split3(x):
    hi = x.astype(BF16)
    rest = x - hi.astype(F32)
    mid = rest.astype(BF16)
    return hi, mid, (rest - mid.astype(F32)).astype(BF16)


def merged(stats, own):
    peers = stats.shape[0]
    top = stats[0]
    for c in range(1, peers):
        top = jnp.maximum(top, stats[c])
    total = jnp.zeros_like(top)
    upper = jnp.zeros_like(top)
    for c in range(peers):
        f = jnp.exp(stats[c] - top)
        total = total + pltpu.roll(stats[c], 128 - PAD, 1) * f
        upper = upper + pltpu.roll(stats[c], 128 - 2 * PAD, 1) * f
    return jnp.exp(own - top) / total, upper / total


def flip(place, bit):
    size = 1 << bit
    return place + size * (1 - 2 * ((place // size) % 2))


def toggled(place, bits):
    for bit in bits:
        place = flip(place, bit)
    return place


def subsets(bits):
    found = [()]
    for bit in bits:
        found = found + [s + (bit,) for s in found]
    return found


def remote(src, dst, send, recv, device):
    return pltpu.make_async_remote_copy(
        src_ref=src,
        dst_ref=dst,
        send_sem=send,
        recv_sem=recv,
        device_id=device,
        device_id_type=pl.DeviceIdType.MESH,
    )


class Scatter:
    def __init__(self, me, data, part, order, slots, send, recv):
        self.me, self.data, self.part, self.order = me, data, part, order
        self.slots, self.send, self.recv = slots, send, recv
        self.sent = []

    def plan(self, phase):
        first = sum(1 << (len(self.order) - 1 - p) for p in range(phase))
        return self.order[phase], list(enumerate(subsets(self.order[phase + 1 :]), first))

    def block(self, owner):
        return self.data.at[(owner, *self.part)]

    def copy(self, phase, slot, bits):
        bit = self.order[phase]
        peer = flip(self.me, bit)
        return remote(
            self.block(toggled(peer, bits)),
            self.slots.at[slot],
            self.send.at[slot],
            self.recv.at[slot],
            {"row": peer},
        )

    def start(self, phase):
        _, blocks = self.plan(phase)
        for slot, bits in blocks:
            copy = self.copy(phase, slot, bits)
            copy.start()
            self.sent.append(copy)

    def finish(self, phase):
        _, blocks = self.plan(phase)
        for slot, bits in blocks:
            self.copy(phase, slot, bits).wait_recv()
            owner = toggled(self.me, bits)
            place = (owner, *self.part)
            self.data[place] = self.data[place] + self.slots[slot]

    def drain(self):
        for copy in self.sent:
            copy.wait_send()


def filled(x, step):
    rest = -x.shape[0] % step
    return jnp.concatenate([x, jnp.zeros((rest, x.shape[1]), F32)], 0) if rest else x


def window(start, size, total):
    return slice(None) if total == size else pl.ds(pl.multiple_of(start, 128), size)


def turned(rot, shift, local, lanes):
    out = []
    for x in range(3):
        total = rot[x, 0:1, lanes] * local(0)
        for y in range(1, 3):
            total = total + rot[x, y : y + 1, lanes] * local(y)
        if shift is not None:
            total = total + shift[x : x + 1, lanes]
        out.append(total)
    return out


def point_coef(head_w, factor):
    x = head_w[...]
    return factor * (jnp.maximum(x, 0.0) + jnp.log(1.0 + jnp.exp(-jnp.abs(x))))


def pick_lane(row, lane):
    mine = lax.broadcasted_iota(jnp.int32, row.shape, 1) == lane
    return jnp.sum(jnp.where(mine, row, 0.0), axis=1, keepdims=True)


def main_kernel(
    shape, limit_ref, pair, bias_in, gpair, head_w, queries, query_points, grad_output,
    grad_points, rot_r, shift_r, rot_c, shift_c, key_in, value_in, key_points, value_points,
    a_out, key_out, key_away, query_out, small_out,
    pair_buf, lbase, dbase, rows_buf, stats, merge_buf, key_rows, key_t, slots_a, slots_b,
    query_rows, query_t, qslots, small, small_col, small_row,
    bias_w, qcat, kcat, gcat, vcat, qraw,
    pair_sem, a_sem, in_sem, stat_send, stat_recv, send_a, recv_a, send_b, recv_b, q_send, q_recv,
    col_send, col_recv, row_send, row_recv,
):
    heads, block, scale, inner, point_factor, nr_dev, nc_dev, nq, nv, vwidth, qsize = shape
    n_rows, cols = pair_buf.shape[0], pair_buf.shape[1]
    blocks = n_rows // block
    me = lax.axis_index("row")
    mc = lax.axis_index("col")
    row_peers = [lax.rem(me + s, nr_dev) for s in range(1, nr_dev)]
    col_peers = [lax.rem(mc + s, nc_dev) for s in range(1, nc_dev)]
    nkp, nvp = key_points.shape[0], value_points.shape[0]
    incoming = [
        pltpu.make_async_copy(key_points, key_rows.at[pl.ds(nvp, nkp)], in_sem.at[0]),
        pltpu.make_async_copy(value_points, key_rows.at[pl.ds(0, nvp)], in_sem.at[1]),
        pltpu.make_async_copy(key_in, kcat.at[:, pl.ds(0, vwidth), :], in_sem.at[2]),
        pltpu.make_async_copy(value_in, vcat.at[:, pl.ds(0, vwidth), :], in_sem.at[3]),
    ]
    for copy in incoming:
        copy.start()

    def load(i):
        rows = pl.ds(pl.multiple_of(i * block, block), block)
        return pltpu.make_async_copy(pair.at[rows], pair_buf.at[rows], pair_sem.at[i])

    def start_load(i, carry):
        load(i).start()
        return carry

    lax.fori_loop(0, blocks, start_load, 0)
    barrier = pltpu.get_barrier_semaphore()
    for peer in row_peers:
        pl.semaphore_signal(
            barrier, inc=1, device_id={"row": peer}, device_id_type=pl.DeviceIdType.MESH
        )
    for peer in col_peers:
        pl.semaphore_signal(
            barrier, inc=1, device_id={"col": peer}, device_id_type=pl.DeviceIdType.MESH
        )

    channels = bias_in.shape[1]
    bias_w[...] = jnp.concatenate(
        [bias_in[...].astype(F32), jnp.zeros((PAD - heads, channels), F32)], 0
    ).astype(BF16)
    coef = point_coef(head_w, point_factor)
    qpoints, vpoints = (qsize - vwidth) // 3, (nv - vwidth) // 3
    span = qsize - vwidth
    lanes = window(me * n_rows, n_rows, rot_r.shape[2])
    qg = turned(rot_r, shift_r, lambda y: query_points[y], lanes)
    gg = turned(rot_r, None, lambda y: grad_points[y], lanes)
    q_square = qg[0] * qg[0] + qg[1] * qg[1] + qg[2] * qg[2]
    for h in range(heads):
        c = pick_lane(coef, h)
        own = slice(vwidth * h, vwidth * h + vwidth)
        points = slice(qpoints * h, qpoints * h + qpoints)
        qcat[h, 0:vwidth] = (scale * inner) * queries[own]
        gcat[h, 0:vwidth] = grad_output[own]
        for x in range(3):
            piece = qg[x][points]
            qraw[h, qpoints * x : qpoints * x + qpoints] = piece
            at = vwidth + qpoints * x
            qcat[h, at : at + qpoints] = (2.0 * c) * piece
            at = vwidth + vpoints * x
            gcat[h, at : at + vpoints] = gg[x][vpoints * h : vpoints * h + vpoints]
        square = jnp.sum(q_square[points], axis=0, keepdims=True)
        qraw[h, span : span + 1] = square
        qcat[h, qsize : qsize + 1] = jnp.broadcast_to(-c, (1, n_rows))
        qcat[h, qsize + 1 : qsize + 2] = -c * square
        qcat[h, qsize + 2 : nq] = jnp.zeros((nq - qsize - 2, n_rows), F32)

    lanes = window(mc * cols, cols, rot_c.shape[2])
    incoming[0].wait()
    incoming[2].wait()
    part = nkp // 3
    kg = turned(rot_c, shift_c, lambda y: key_rows[nvp + part * y : nvp + part * y + part], lanes)
    k_square = kg[0] * kg[0] + kg[1] * kg[1] + kg[2] * kg[2]
    for h in range(heads):
        points = slice(qpoints * h, qpoints * h + qpoints)
        for x in range(3):
            at = vwidth + qpoints * x
            kcat[h, at : at + qpoints] = kg[x][points]
        kcat[h, qsize : qsize + 1] = jnp.sum(k_square[points], axis=0, keepdims=True)
        kcat[h, qsize + 1 : qsize + 2] = jnp.ones((1, cols), F32)
        kcat[h, qsize + 2 : nq] = jnp.zeros((nq - qsize - 2, cols), F32)
    incoming[1].wait()
    incoming[3].wait()
    part_v = nvp // 3
    vg = turned(rot_c, shift_c, lambda y: key_rows[part_v * y : part_v * y + part_v], lanes)
    for h in range(heads):
        for x in range(3):
            at = vwidth + vpoints * x
            vcat[h, at : at + vpoints] = vg[x][vpoints * h : vpoints * h + vpoints]

    def base(h, carry):
        q0, q1, q2 = split3(qcat[h])
        k0, k1, k2 = split3(kcat[h])
        lbase[h] = dot(
            jnp.concatenate([q0, q0, q1, q0, q2, q1], 0),
            jnp.concatenate([k0, k1, k0, k2, k0, k1], 0),
            TN,
        )
        g0, g1 = split2(filled(gcat[h], PAD))
        v0, v1 = split2(filled(vcat[h], PAD))
        dbase[h] = dot(
            jnp.concatenate([g0, g0, g1], 0), jnp.concatenate([v0, v1, v0], 0), TN
        )
        return carry

    lax.fori_loop(0, heads, base, 0)
    limit = limit_ref[0] - mc * cols
    valid = lax.broadcasted_iota(jnp.int32, (block, cols), 1) < limit
    lane = lax.broadcasted_iota(jnp.int32, (block, 128), 1)

    def forward(i, carry):
        load(i).wait()
        first = pl.multiple_of(i * block, block)
        rows = pl.ds(first, block)
        for r in range(block):
            w = jnp.concatenate([bias_w[...], gpair[first + r]], 0)
            rows_buf[r] = dot(w, pair_buf[first + r], NT)
        packed = jnp.ones((block, 128), F32)
        for h in range(heads):
            logit = lbase[h, rows, :] + scale * rows_buf[:, h, :]
            logit = jnp.where(valid, logit, F32(-1000000000.0))
            peak = jnp.max(logit, axis=1, keepdims=True)
            e = jnp.exp(logit - peak)
            d = dbase[h, rows, :] + rows_buf[:, PAD + h, :]
            lbase[h, rows, :] = e
            dbase[h, rows, :] = d
            packed = jnp.where(lane == h, peak, packed)
            packed = jnp.where(lane == PAD + h, jnp.sum(e, axis=1, keepdims=True), packed)
            packed = jnp.where(
                lane == 2 * PAD + h, jnp.sum(e * d, axis=1, keepdims=True), packed
            )
        stats[0, rows, :] = packed
        return carry

    lax.fori_loop(0, blocks, forward, 0)

    pl.semaphore_wait(barrier, nr_dev + nc_dev - 2)
    sent = []

    def stat_copy(s, peer):
        return remote(
            stats.at[0], stats.at[s], stat_send.at[s], stat_recv.at[s], {"col": peer}
        )

    for s, peer in enumerate(col_peers, 1):
        copy = stat_copy(s, peer)
        copy.start()
        sent.append(copy)
    for s, peer in enumerate(col_peers, 1):
        stat_copy(s, peer).wait_recv()
    factor, delta = merged(stats, stats[0])
    merge_buf[0] = factor
    merge_buf[1] = delta

    lane_of = lax.broadcasted_iota(jnp.int32, (n_rows, 128), 1)
    row_of = lax.broadcasted_iota(jnp.int32, (PAD, 128), 0)
    lane_small = lax.broadcasted_iota(jnp.int32, (PAD, 128), 1)
    small[...] = jnp.zeros_like(small)
    key_rows[...] = jnp.zeros_like(key_rows)
    query_rows[...] = jnp.zeros_like(query_rows)

    def sums(h, carry):
        mine = lane_of == h
        pick = lambda x: jnp.sum(jnp.where(mine, x, 0.0), axis=1, keepdims=True)
        att = lbase[h] * pick(merge_buf[0])
        dl = att * (dbase[h] - pick(merge_buf[1]))
        a0 = att.astype(BF16)
        d0, d1 = split2(dl)
        q = jnp.concatenate(split2(qcat[h]), 0)
        k = jnp.concatenate(split2(kcat[h]), 0)
        g = jnp.concatenate(split2(filled(gcat[h], PAD)), 0)
        v = jnp.concatenate(split2(filled(vcat[h], PAD)), 0)
        kk = dot(q, d0, NN) + dot(q, d1, NN)
        vv = dot(g, a0, NN)
        half = g.shape[0] // 2
        first = pl.multiple_of(h * (nq + nv), 8)
        key_rows[pl.ds(first, nq), :] = kk[:nq] + kk[nq:]
        key_rows[pl.ds(first + nq, nv), :] = vv[:nv] + vv[half : half + nv]
        qq = dot(k, d0, NT) + dot(k, d1, NT)
        qq = qq[:nq] + qq[nq:]
        oo = dot(v, a0, NT)
        first = pl.multiple_of(h * (nq + nv - vwidth), 8)
        query_rows[pl.ds(first, nq), :] = qq
        query_rows[pl.ds(first + nq, nv - vwidth), :] = (
            oo[vwidth:nv] + oo[half + vwidth : half + nv]
        )
        raw = qraw[h]
        span = qsize - vwidth
        part = raw[span : span + 1] * qq[qsize + 1 : qsize + 2] + qq[qsize : qsize + 1]
        part = part - 2.0 * jnp.sum(raw[:span] * qq[vwidth:qsize], axis=0, keepdims=True)
        part = jnp.sum(part, axis=1, keepdims=True)
        small[...] = small[...] + jnp.where(
            (row_of == heads) & (lane_small == h), part, 0.0
        )
        return carry

    lax.fori_loop(0, heads, sums, 0)

    share = cols // nr_dev
    for t in range(key_t.shape[2] // 128):
        part = slice(128 * t, 128 * t + 128)
        key_t[:, :, part] = key_rows[part, :].T.reshape(nr_dev, share, 128)
    qshare = n_rows // nc_dev
    for t in range(query_t.shape[2] // 128):
        part = slice(128 * t, 128 * t + 128)
        query_t[:, :, part] = query_rows[part, :].T.reshape(nc_dev, qshare, 128)

    bits = list(range(nr_dev.bit_length() - 1))
    swapped = bits[:1] + bits[1:3][::-1] + bits[3:]
    lane_count = key_t.shape[2]
    if slots_a.shape[2] == lane_count:
        cut = slots_a.shape[1]
        parts = [(pl.ds(0, cut), slice(None)), (pl.ds(cut, share - cut), slice(None))]
    else:
        cut = slots_a.shape[2]
        parts = [(slice(None), pl.ds(0, cut)), (slice(None), pl.ds(cut, lane_count - cut))]
    streams = [
        Scatter(me, key_t, parts[0], bits, slots_a, send_a, recv_a),
        Scatter(me, key_t, parts[1], swapped, slots_b, send_b, recv_b),
    ]
    last = len(bits) - 1

    def q_copy(s, peer):
        return remote(
            query_t.at[peer], qslots.at[s], q_send.at[s], q_recv.at[s], {"col": peer}
        )

    for s, peer in enumerate(col_peers):
        copy = q_copy(s, peer)
        copy.start()
        sent.append(copy)
    for stream in streams:
        if last > 0:
            stream.start(0)

    rows_buf[...] = jnp.zeros_like(rows_buf)

    depth = a_out.shape[1]

    def a_copy(i):
        rows = pl.ds(pl.multiple_of(i * block, block), block)
        return pltpu.make_async_copy(
            pair_buf.at[rows, pl.ds(0, depth), :], a_out.at[rows], a_sem.at[i]
        )

    def weights(i, carry):
        first = pl.multiple_of(i * block, block)
        rows = pl.ds(first, block)
        factor = merge_buf[0, rows, :]
        delta = merge_buf[1, rows, :]
        for h in range(heads):
            att = lbase[h, rows, :] * factor[:, h : h + 1]
            rows_buf[:, h, :] = att * (dbase[h, rows, :] - delta[:, h : h + 1])
            rows_buf[:, PAD + h, :] = att
        acc = small[...]
        for r in range(block):
            a = rows_buf[r].astype(BF16)
            acc = acc + scale * dot(a[:PAD], pair_buf[first + r], NN)
            for c in range(cols // 128):
                pair_buf[first + r, 2 * PAD * c : 2 * PAD * c + 2 * PAD, :] = a[
                    :, 128 * c : 128 * c + 128
                ]
        small[...] = acc

        @pl.when(i > 0)
        def _():
            a_copy(i - 1).start()

        return carry

    early = blocks // 4
    lax.fori_loop(0, early, weights, 0)
    for stream in streams:
        if last > 0:
            stream.finish(0)
        if last > 1:
            stream.start(1)
    lax.fori_loop(early, blocks, weights, 0)
    a_copy(blocks - 1).start()

    def col_copy(s, peer):
        return remote(
            small, small_col.at[s], col_send.at[s], col_recv.at[s], {"col": peer}
        )

    for s, peer in enumerate(col_peers):
        copy = col_copy(s, peer)
        copy.start()
        sent.append(copy)
    total = query_t[mc]
    for s, peer in enumerate(col_peers):
        q_copy(s, peer).wait_recv()
        total = total + qslots[s]
    query_t[mc] = total

    for stream in streams:
        if last > 1:
            stream.finish(1)
        if last > 2:
            stream.start(2)

    total = small[...]
    for s, peer in enumerate(col_peers):
        col_copy(s, peer).wait_recv()
        total = total + small_col[s]
    small_row[0] = total

    def row_copy(s, peer):
        return remote(
            small_row.at[0], small_row.at[s], row_send.at[s], row_recv.at[s], {"row": peer}
        )

    for s, peer in enumerate(row_peers, 1):
        copy = row_copy(s, peer)
        copy.start()
        sent.append(copy)
    for phase in range(2, last):
        for stream in streams:
            stream.finish(phase)
            if phase + 1 < last:
                stream.start(phase + 1)
    leaving = [
        pltpu.make_async_copy(key_t.at[me], key_out, in_sem.at[0]),
        pltpu.make_async_copy(key_t.at[flip(me, last)], key_away, in_sem.at[1]),
        pltpu.make_async_copy(query_t.at[mc], query_out, in_sem.at[2]),
    ]
    total = small_row[0]
    for s, peer in enumerate(row_peers, 1):
        row_copy(s, peer).wait_recv()
        total = total + small_row[s]
    small_out[...] = total
    for copy in leaving:
        copy.start()
    for copy in sent:
        copy.wait_send()
    for copy in leaving:
        copy.wait()
    for stream in streams:
        stream.drain()

    def end_copy(i, carry):
        a_copy(i).wait()
        return carry

    lax.fori_loop(0, blocks, end_copy, 0)


def pair_kernel(block, scale, a_in, bias_in, gpair, pg_out):
    heads, channels = bias_in.shape
    w_hi, w_lo = split2(
        jnp.concatenate(
            [scale * bias_in[...].astype(F32), jnp.zeros((PAD - heads, channels), F32)], 0
        )
    )
    for r in range(block):
        step = 2 * PAD
        a = jnp.concatenate(
            [a_in[r, at : at + step, :] for at in range(0, a_in.shape[1], step)], 1
        )
        lhs = jnp.concatenate([a, a[:PAD]], 0)
        rhs = jnp.concatenate([w_hi, gpair[r], w_lo], 0)
        pg_out[r] = dot(lhs, rhs, TN).astype(BF16)


def own_lanes(load, start, size, total):
    if total == size:
        return load(slice(None))
    first = pl.multiple_of((start // 128) * 128, 128)
    tile = load(pl.ds(first, 128))
    return pltpu.roll(tile, lax.rem(128 - lax.rem(start, 128), 128), 1)[:, :size]


def upright(ref, rows):
    for t in range(rows.shape[0] // 128):
        part = slice(128 * t, 128 * t + 128)
        rows[part, :] = ref(part).T


def tail_kernel(
    shape, key_own, key_more, query_part, small, head_w, rot, shift, query_points, grad_points,
    key_points, value_points,
    query_grad, query_point_grad, query_frame, key_grad, value_grad, key_point_grad,
    value_point_grad, key_frame, weight_total, head_grad,
    krows, qrows, dpoint, dvalue, wide,
):
    heads, scale, inner, point_factor, nq, nv, vwidth, qsize = shape
    qpoints, vpoints = (qsize - vwidth) // 3, (nv - vwidth) // 3
    me = lax.axis_index("row")
    mc = lax.axis_index("col")
    coef = point_coef(head_w, point_factor)
    weight_total[...] = small[:heads, :]
    x = head_w[...]
    grads = small[heads : heads + 1, :heads]
    slope = -point_factor
    head_grad[...] = grads * slope / (1.0 + jnp.exp(-x))

    def flat(source, out):
        rows = source.shape[0]
        wide[0:rows, 0 : source.shape[1]] = source
        for t in range(wide.shape[0] // 128):
            piece = wide[128 * t : 128 * t + 128, :].T
            end = min(128, rows - 128 * t)
            if end > 0:
                out(slice(128 * t, 128 * t + end), piece[: source.shape[1], :end])

    wide[...] = jnp.zeros_like(wide)

    def put(ref):
        def store(lanes, value):
            ref[:, lanes] = value

        return store

    share = query_part.shape[0]
    upright(lambda part: query_part[:, part], qrows)
    start = mc * share
    base = me * (share * lax.axis_size("col")) + start
    total = rot.shape[2]
    turns = [
        [own_lanes(lambda s: rot[i, j : j + 1, s], base, share, total) for j in range(3)]
        for i in range(3)
    ]
    shifts = [own_lanes(lambda s: shift[i : i + 1, s], base, share, total) for i in range(3)]
    local = [
        own_lanes(lambda s: query_points[y, :, s], start, share, query_points.shape[2])
        for y in range(3)
    ]
    cotan = [
        own_lanes(lambda s: grad_points[y, :, s], start, share, grad_points.shape[2])
        for y in range(3)
    ]
    nr = nq + nv - vwidth
    flat(
        (scale * inner)
        * jnp.concatenate([qrows[nr * h : nr * h + vwidth] for h in range(heads)], 0),
        put(query_grad),
    )
    spin = lambda i, v: turns[i][0] * v[0] + turns[i][1] * v[1] + turns[i][2] * v[2]
    for i in range(3):
        qg = spin(i, local) + shifts[i]
        for h in range(heads):
            points = slice(qpoints * h, qpoints * h + qpoints)
            at = nr * h + vwidth + qpoints * i
            sums = qrows[nr * h + qsize + 1 : nr * h + qsize + 2]
            dpoint[i, points] = (-2.0 * pick_lane(coef, h)) * (
                qg[points] * sums - qrows[at : at + qpoints]
            )
            at = nr * h + nq + vpoints * i
            dvalue[i, vpoints * h : vpoints * h + vpoints] = qrows[at : at + vpoints]
    down = lambda v: jnp.sum(v, axis=0, keepdims=True)
    for y in range(3):
        query_point_grad[y] = (
            turns[0][y] * dpoint[0] + turns[1][y] * dpoint[1] + turns[2][y] * dpoint[2]
        )
    for i in range(3):
        away = dvalue[i] - shifts[i]
        for y in range(3):
            query_frame[i, y : y + 1] = down(dpoint[i] * local[y]) + down(away * cotan[y])
        query_frame[i, 3:4] = down(dpoint[i]) - down(spin(i, cotan))

    share = key_own.shape[0]
    upright(lambda part: key_own[:, part] + key_more[:, part], krows)
    start = me * share
    base = mc * (share * lax.axis_size("row")) + start
    turns = [
        [own_lanes(lambda s: rot[i, j : j + 1, s], base, share, total) for j in range(3)]
        for i in range(3)
    ]
    shifts = [own_lanes(lambda s: shift[i : i + 1, s], base, share, total) for i in range(3)]
    local = [
        own_lanes(lambda s: key_points[y, :, s], start, share, key_points.shape[2])
        for y in range(3)
    ]
    values = [
        own_lanes(lambda s: value_points[y, :, s], start, share, value_points.shape[2])
        for y in range(3)
    ]
    nk = nq + nv
    flat(jnp.concatenate([krows[nk * h : nk * h + vwidth] for h in range(heads)], 0), put(key_grad))
    flat(
        jnp.concatenate([krows[nk * h + nq : nk * h + nq + vwidth] for h in range(heads)], 0),
        put(value_grad),
    )
    for i in range(3):
        kg = spin(i, local) + shifts[i]
        for h in range(heads):
            points = slice(qpoints * h, qpoints * h + qpoints)
            at = nk * h + vwidth + qpoints * i
            sums = krows[nk * h + qsize : nk * h + qsize + 1]
            dpoint[i, points] = krows[at : at + qpoints] + 2.0 * kg[points] * sums
            at = nk * h + nq + vwidth + vpoints * i
            dvalue[i, vpoints * h : vpoints * h + vpoints] = krows[at : at + vpoints]
    for y in range(3):
        key_point_grad[y] = (
            turns[0][y] * dpoint[0] + turns[1][y] * dpoint[1] + turns[2][y] * dpoint[2]
        )
        flat(
            turns[0][y] * dvalue[0] + turns[1][y] * dvalue[1] + turns[2][y] * dvalue[2],
            put(value_point_grad.at[y]),
        )
    for i in range(3):
        for y in range(3):
            key_frame[i, y : y + 1] = down(dpoint[i] * local[y]) + down(dvalue[i] * values[y])
        key_frame[i, 3:4] = down(dpoint[i]) + down(dvalue[i])


def pad_rows(x, rows):
    return jnp.pad(x, ((0, 0), (0, rows - x.shape[1]), (0, 0)))


def per_device(
    pair_rep, bias_weight, head_weight, queries, key_vectors, values, query_points, key_points,
    value_points, rotations, translations, residue_count, grad_output, grad_points, grad_pair,
):
    channels, heads = bias_weight.shape
    width = queries.shape[0] // heads
    qpoints = query_points.shape[1] // heads
    vpoints = value_points.shape[1] // heads
    n_rows = queries.shape[1]
    n_cols = key_vectors.shape[1]
    logit_scale = math.sqrt(1.0 / 3.0)
    point_scale = math.sqrt(2.0 / (9.0 * qpoints))
    inner_scale = 1.0 / math.sqrt(width)
    point_factor = 0.5 * logit_scale * point_scale
    qsize = width + 3 * qpoints
    nq = -(-(qsize + 2) // 16) * 16
    nv = width + 3 * vpoints
    bias_t = bias_weight.T
    gpair = pad_rows(grad_pair, PAD)
    head_row = head_weight.reshape(1, heads)

    block = 8
    depth = n_cols // 128 * 2 * PAD
    rows_dev = lax.axis_size("row")
    cols_dev = lax.axis_size("col")
    nk = nq + nv
    nr = nq + nv - width
    key_lanes = -(-heads * nk // 128) * 128
    query_lanes = -(-heads * nr // 128) * 128
    kshare = n_cols // rows_dev
    qshare = n_rows // cols_dev
    slot_count = max(rows_dev - 2, 1)
    if kshare % 16 == 0:
        slot_shapes = [(slot_count, kshare // 2, key_lanes)] * 2
    else:
        cut = -(-key_lanes // 256) * 128
        slot_shapes = [(slot_count, kshare, c) for c in (cut, key_lanes - cut)]
    rot_rows, shift_rows = rotations, translations
    if n_rows % 128:
        row_start = lax.axis_index("row") * n_rows
        rot_rows = lax.dynamic_slice_in_dim(rotations, row_start, n_rows, 2)
        shift_rows = lax.dynamic_slice_in_dim(translations, row_start, n_rows, 1)
    vmem = pl.BlockSpec(memory_space=pltpu.VMEM)
    anywhere = pl.BlockSpec(memory_space=pl.ANY)
    sems = lambda count: pltpu.SemaphoreType.DMA((max(count, 1),))
    a_all, key_own, key_away, query_part, small = pl.pallas_call(
        functools.partial(
            main_kernel,
            (
                heads, block, logit_scale, inner_scale, point_factor, rows_dev, cols_dev,
                nq, nv, width, qsize,
            ),
        ),
        in_specs=[pl.BlockSpec(memory_space=pltpu.SMEM), anywhere] + [vmem] * 11 + [anywhere] * 4,
        out_specs=[anywhere] * 4 + [vmem],
        out_shape=[
            jax.ShapeDtypeStruct((n_rows, depth, 128), BF16),
            jax.ShapeDtypeStruct((kshare, key_lanes), F32),
            jax.ShapeDtypeStruct((kshare, key_lanes), F32),
            jax.ShapeDtypeStruct((qshare, query_lanes), F32),
            jax.ShapeDtypeStruct((PAD, channels), F32),
        ],
        scratch_shapes=[
            pltpu.VMEM((n_rows, n_cols, channels), BF16),
            pltpu.VMEM((heads, n_rows, n_cols), F32),
            pltpu.VMEM((heads, n_rows, n_cols), F32),
            pltpu.VMEM((block, 2 * PAD, n_cols), F32),
            pltpu.VMEM((cols_dev, n_rows, 128), F32),
            pltpu.VMEM((2, n_rows, 128), F32),
            pltpu.VMEM((key_lanes, n_cols), F32),
            pltpu.VMEM((rows_dev, kshare, key_lanes), F32),
            pltpu.VMEM(slot_shapes[0], F32),
            pltpu.VMEM(slot_shapes[1], F32),
            pltpu.VMEM((query_lanes, n_rows), F32),
            pltpu.VMEM((cols_dev, qshare, query_lanes), F32),
            pltpu.VMEM((max(cols_dev - 1, 1), qshare, query_lanes), F32),
            pltpu.VMEM((PAD, channels), F32),
            pltpu.VMEM((max(cols_dev - 1, 1), PAD, channels), F32),
            pltpu.VMEM((rows_dev, PAD, channels), F32),
            pltpu.VMEM((PAD, channels), BF16),
            pltpu.VMEM((heads, nq, n_rows), F32),
            pltpu.VMEM((heads, nq, n_cols), F32),
            pltpu.VMEM((heads, nv, n_rows), F32),
            pltpu.VMEM((heads, nv, n_cols), F32),
            pltpu.VMEM((heads, PAD, n_rows), F32),
            sems(n_rows // block),
            sems(n_rows // block),
            sems(4),
            sems(cols_dev),
            sems(cols_dev),
            sems(rows_dev - 1),
            sems(rows_dev - 1),
            sems(rows_dev - 1),
            sems(rows_dev - 1),
            sems(cols_dev - 1),
            sems(cols_dev - 1),
            sems(cols_dev - 1),
            sems(cols_dev - 1),
            sems(rows_dev),
            sems(rows_dev),
        ],
        compiler_params=pltpu.CompilerParams(
            collective_id=0, has_side_effects=True, vmem_limit_bytes=VMEM_LIMIT
        ),
    )(
        residue_count, pair_rep, bias_t, gpair, head_row, queries, query_points, grad_output,
        grad_points, rot_rows, shift_rows, rotations, translations,
        key_vectors.reshape(heads, width, n_cols), values.reshape(heads, width, n_cols),
        key_points.reshape(-1, n_cols), value_points.reshape(-1, n_cols),
    )
    half = rows_dev // 2
    key_more = lax.ppermute(key_away, "row", [(i, (i + half) % rows_dev) for i in range(rows_dev)])

    out_block = 16
    pair_grad = pl.pallas_call(
        functools.partial(pair_kernel, out_block, logit_scale),
        grid=(n_rows // out_block,),
        in_specs=[
            pl.BlockSpec((out_block, depth, 128), lambda i: (i, 0, 0)),
            pl.BlockSpec((heads, channels), lambda i: (0, 0)),
            pl.BlockSpec((out_block, PAD, channels), lambda i: (i, 0, 0)),
        ],
        out_specs=pl.BlockSpec((out_block, n_cols, channels), lambda i: (i, 0, 0)),
        out_shape=jax.ShapeDtypeStruct(pair_rep.shape, BF16),
        compiler_params=pltpu.CompilerParams(dimension_semantics=("arbitrary",)),
        cost_estimate=pl.CostEstimate(
            flops=4 * n_rows * n_cols * channels * PAD,
            bytes_accessed=2 * n_rows * n_cols * (channels + 2 * PAD),
            transcendentals=0,
        ),
    )(a_all, bias_t, gpair)

    local_q, local_g = query_points, grad_points
    if n_rows % 128:
        start = lax.axis_index("col") * qshare
        local_q = lax.dynamic_slice_in_dim(query_points, start, qshare, 2)
        local_g = lax.dynamic_slice_in_dim(grad_points, start, qshare, 2)
    most = max(kshare, qshare, 128)
    f32 = lambda *dims: jax.ShapeDtypeStruct(dims, F32)
    (
        query_grad, query_point_grad, query_frame_grad, key_grad, value_grad, key_point_grad,
        value_point_grad, key_frame_grad, weight_total, head_weight_grad,
    ) = pl.pallas_call(
        functools.partial(
            tail_kernel,
            (heads, logit_scale, inner_scale, point_factor, nq, nv, width, qsize),
        ),
        in_specs=[vmem] * 11,
        out_specs=[vmem] * 10,
        out_shape=[
            f32(qshare, heads * width),
            f32(3, heads * qpoints, qshare),
            f32(3, 4, qshare),
            f32(kshare, heads * width),
            f32(kshare, heads * width),
            f32(3, heads * qpoints, kshare),
            f32(3, kshare, heads * vpoints),
            f32(3, 4, kshare),
            f32(heads, channels),
            f32(1, heads),
        ],
        scratch_shapes=[
            pltpu.VMEM((key_lanes, kshare), F32),
            pltpu.VMEM((query_lanes, qshare), F32),
            pltpu.VMEM((3, heads * qpoints, kshare), F32),
            pltpu.VMEM((3, heads * vpoints, kshare), F32),
            pltpu.VMEM((-(-heads * width // 128) * 128, most), F32),
        ],
    )(
        key_own, key_more, query_part, small, head_row, rotations, translations, local_q,
        local_g, key_points, value_points,
    )
    query_grad, key_grad, value_grad = query_grad.T, key_grad.T, value_grad.T
    value_point_grad = value_point_grad.transpose(0, 2, 1)
    weight_total, head_weight_grad = weight_total.T, head_weight_grad.reshape(heads)
    return (
        pair_grad, query_grad, query_point_grad, query_frame_grad, key_grad, value_grad,
        key_point_grad, value_point_grad, key_frame_grad, weight_total, head_weight_grad,
    )


def solution(mesh):
    return jax.shard_map(
        per_device,
        mesh=mesh,
        in_specs=(
            P("row", "col", None),
            P(),
            P(),
            P(None, "row"),
            P(None, "col"),
            P(None, "col"),
            P(None, None, "row"),
            P(None, None, "col"),
            P(None, None, "col"),
            P(),
            P(),
            P(),
            P(None, "row"),
            P(None, None, "row"),
            P("row", None, None),
        ),
        out_specs=(
            P("row", "col", None),
            P(None, ("row", "col")),
            P(None, None, ("row", "col")),
            P(None, None, ("row", "col")),
            P(None, ("col", "row")),
            P(None, ("col", "row")),
            P(None, None, ("col", "row")),
            P(None, None, ("col", "row")),
            P(None, None, ("col", "row")),
            P(),
            P(),
        ),
        check_vma=False,
    )
```

```python
import functools
import math

import jax
import jax.numpy as jnp
from jax import lax
from jax.experimental import pallas as pl
from jax.experimental.pallas import tpu as pltpu
from jax.sharding import PartitionSpec as P

F32 = jnp.float32
BF16 = jnp.bfloat16
PAD = 16
VMEM_LIMIT = 67043328


def dot(a, b, dims):
    return lax.dot_general(a, b, (dims, ((), ())), preferred_element_type=F32)


TN = ((0,), (0,))
NT = ((1,), (1,))
NN = ((1,), (0,))


def split2(x):
    hi = x.astype(BF16)
    return hi, (x - hi.astype(F32)).astype(BF16)


def split3(x):
    hi = x.astype(BF16)
    rest = x - hi.astype(F32)
    mid = rest.astype(BF16)
    return hi, mid, (rest - mid.astype(F32)).astype(BF16)


def merged(stats, own):
    peers = stats.shape[0]
    top = stats[0]
    for c in range(1, peers):
        top = jnp.maximum(top, stats[c])
    total = jnp.zeros_like(top)
    upper = jnp.zeros_like(top)
    for c in range(peers):
        f = jnp.exp(stats[c] - top)
        total = total + pltpu.roll(stats[c], 128 - PAD, 1) * f
        upper = upper + pltpu.roll(stats[c], 128 - 2 * PAD, 1) * f
    return jnp.exp(own - top) / total, upper / total


def flip(place, bit):
    size = 1 << bit
    return place + size * (1 - 2 * ((place // size) % 2))


def toggled(place, bits):
    for bit in bits:
        place = flip(place, bit)
    return place


def subsets(bits):
    found = [()]
    for bit in bits:
        found = found + [s + (bit,) for s in found]
    return found


def remote(src, dst, send, recv, device):
    return pltpu.make_async_remote_copy(
        src_ref=src,
        dst_ref=dst,
        send_sem=send,
        recv_sem=recv,
        device_id=device,
        device_id_type=pl.DeviceIdType.MESH,
    )


class Scatter:
    def __init__(self, me, data, part, order, slots, send, recv):
        self.me, self.data, self.part, self.order = me, data, part, order
        self.slots, self.send, self.recv = slots, send, recv
        self.sent = []

    def plan(self, phase):
        first = sum(1 << (len(self.order) - 1 - p) for p in range(phase))
        return self.order[phase], list(enumerate(subsets(self.order[phase + 1 :]), first))

    def block(self, owner):
        return self.data.at[(owner, *self.part)]

    def copy(self, phase, slot, bits):
        bit = self.order[phase]
        peer = flip(self.me, bit)
        return remote(
            self.block(toggled(peer, bits)),
            self.slots.at[slot],
            self.send.at[slot],
            self.recv.at[slot],
            {"row": peer},
        )

    def start(self, phase):
        _, blocks = self.plan(phase)
        for slot, bits in blocks:
            copy = self.copy(phase, slot, bits)
            copy.start()
            self.sent.append(copy)

    def finish(self, phase):
        _, blocks = self.plan(phase)
        for slot, bits in blocks:
            self.copy(phase, slot, bits).wait_recv()
            owner = toggled(self.me, bits)
            place = (owner, *self.part)
            self.data[place] = self.data[place] + self.slots[slot]

    def drain(self):
        for copy in self.sent:
            copy.wait_send()


def filled(x, step):
    rest = -x.shape[0] % step
    return jnp.concatenate([x, jnp.zeros((rest, x.shape[1]), F32)], 0) if rest else x


def window(start, size, total):
    return slice(None) if total == size else pl.ds(pl.multiple_of(start, 128), size)


def turned(rot, shift, local, lanes):
    out = []
    for x in range(3):
        total = rot[x, 0:1, lanes] * local(0)
        for y in range(1, 3):
            total = total + rot[x, y : y + 1, lanes] * local(y)
        if shift is not None:
            total = total + shift[x : x + 1, lanes]
        out.append(total)
    return out


def point_coef(head_w, factor):
    x = head_w[...]
    return factor * (jnp.maximum(x, 0.0) + jnp.log(1.0 + jnp.exp(-jnp.abs(x))))


def pick_lane(row, lane):
    mine = lax.broadcasted_iota(jnp.int32, row.shape, 1) == lane
    return jnp.sum(jnp.where(mine, row, 0.0), axis=1, keepdims=True)


def main_kernel(
    shape, limit_ref, pair, bias_in, gpair, head_w, queries, query_points, grad_output,
    grad_points, rot_r, shift_r, rot_c, shift_c, key_in, value_in, key_points, value_points,
    a_out, key_out, key_away, query_out, small_out,
    pair_buf, lbase, dbase, rows_buf, stats, merge_buf, key_rows, key_t, slots,
    query_rows, query_t, qslots, small, small_col, small_row,
    bias_w, qcat, kcat, gcat, vcat, qraw,
    pair_sem, a_sem, in_sem, stat_send, stat_recv, key_send, key_recv, q_send, q_recv,
    col_send, col_recv, row_send, row_recv,
):
    heads, block, scale, inner, point_factor, nr_dev, nc_dev, nq, nv, vwidth, qsize, lead = shape
    n_rows, cols = pair_buf.shape[0], pair_buf.shape[1]
    blocks = n_rows // block
    me = lax.axis_index("row")
    mc = lax.axis_index("col")
    row_peers = [lax.rem(me + s, nr_dev) for s in range(1, nr_dev)]
    col_peers = [lax.rem(mc + s, nc_dev) for s in range(1, nc_dev)]
    nkp, nvp = key_points.shape[0], value_points.shape[0]
    incoming = [
        pltpu.make_async_copy(key_points, key_rows.at[pl.ds(nvp, nkp)], in_sem.at[0]),
        pltpu.make_async_copy(value_points, key_rows.at[pl.ds(0, nvp)], in_sem.at[1]),
        pltpu.make_async_copy(key_in, kcat.at[:, pl.ds(0, vwidth), :], in_sem.at[2]),
        pltpu.make_async_copy(value_in, vcat.at[:, pl.ds(0, vwidth), :], in_sem.at[3]),
    ]
    for copy in incoming:
        copy.start()

    def load(i):
        rows = pl.ds(pl.multiple_of(i * block, block), block)
        return pltpu.make_async_copy(pair.at[rows], pair_buf.at[rows], pair_sem.at[i])

    def start_load(i, carry):
        load(i).start()
        return carry

    lax.fori_loop(0, blocks, start_load, 0)
    barrier = pltpu.get_barrier_semaphore()
    for peer in row_peers:
        pl.semaphore_signal(
            barrier, inc=1, device_id={"row": peer}, device_id_type=pl.DeviceIdType.MESH
        )
    for peer in col_peers:
        pl.semaphore_signal(
            barrier, inc=1, device_id={"col": peer}, device_id_type=pl.DeviceIdType.MESH
        )

    channels = bias_in.shape[1]
    bias_w[...] = jnp.concatenate(
        [bias_in[...].astype(F32), jnp.zeros((PAD - heads, channels), F32)], 0
    ).astype(BF16)
    coef = point_coef(head_w, point_factor)
    qpoints, vpoints = (qsize - vwidth) // 3, (nv - vwidth) // 3
    span = qsize - vwidth
    lanes = window(me * n_rows, n_rows, rot_r.shape[2])
    qg = turned(rot_r, shift_r, lambda y: query_points[y], lanes)
    gg = turned(rot_r, None, lambda y: grad_points[y], lanes)
    q_square = qg[0] * qg[0] + qg[1] * qg[1] + qg[2] * qg[2]
    for h in range(heads):
        c = pick_lane(coef, h)
        own = slice(vwidth * h, vwidth * h + vwidth)
        points = slice(qpoints * h, qpoints * h + qpoints)
        qcat[h, 0:vwidth] = (scale * inner) * queries[own]
        gcat[h, 0:vwidth] = grad_output[own]
        for x in range(3):
            piece = qg[x][points]
            qraw[h, qpoints * x : qpoints * x + qpoints] = piece
            at = vwidth + qpoints * x
            qcat[h, at : at + qpoints] = (2.0 * c) * piece
            at = vwidth + vpoints * x
            gcat[h, at : at + vpoints] = gg[x][vpoints * h : vpoints * h + vpoints]
        square = jnp.sum(q_square[points], axis=0, keepdims=True)
        qraw[h, span : span + 1] = square
        qcat[h, qsize : qsize + 1] = jnp.broadcast_to(-c, (1, n_rows))
        qcat[h, qsize + 1 : qsize + 2] = -c * square
        qcat[h, qsize + 2 : nq] = jnp.zeros((nq - qsize - 2, n_rows), F32)

    lanes = window(mc * cols, cols, rot_c.shape[2])
    incoming[0].wait()
    incoming[2].wait()
    part = nkp // 3
    kg = turned(rot_c, shift_c, lambda y: key_rows[nvp + part * y : nvp + part * y + part], lanes)
    k_square = kg[0] * kg[0] + kg[1] * kg[1] + kg[2] * kg[2]
    for h in range(heads):
        points = slice(qpoints * h, qpoints * h + qpoints)
        for x in range(3):
            at = vwidth + qpoints * x
            kcat[h, at : at + qpoints] = kg[x][points]
        kcat[h, qsize : qsize + 1] = jnp.sum(k_square[points], axis=0, keepdims=True)
        kcat[h, qsize + 1 : qsize + 2] = jnp.ones((1, cols), F32)
        kcat[h, qsize + 2 : nq] = jnp.zeros((nq - qsize - 2, cols), F32)
    incoming[1].wait()
    incoming[3].wait()
    part_v = nvp // 3
    vg = turned(rot_c, shift_c, lambda y: key_rows[part_v * y : part_v * y + part_v], lanes)
    for h in range(heads):
        for x in range(3):
            at = vwidth + vpoints * x
            vcat[h, at : at + vpoints] = vg[x][vpoints * h : vpoints * h + vpoints]

    def base(h, carry):
        q0, q1, q2 = split3(qcat[h])
        k0, k1, k2 = split3(kcat[h])
        lbase[h] = dot(
            jnp.concatenate([q0, q0, q1, q0, q2, q1], 0),
            jnp.concatenate([k0, k1, k0, k2, k0, k1], 0),
            TN,
        )
        g0, g1 = split2(filled(gcat[h], PAD))
        v0, v1 = split2(filled(vcat[h], PAD))
        dbase[h] = dot(
            jnp.concatenate([g0, g0, g1], 0), jnp.concatenate([v0, v1, v0], 0), TN
        )
        return carry

    lax.fori_loop(0, heads, base, 0)
    limit = limit_ref[0] - mc * cols
    valid = lax.broadcasted_iota(jnp.int32, (block, cols), 1) < limit
    lane = lax.broadcasted_iota(jnp.int32, (block, 128), 1)

    def forward(i, carry):
        load(i).wait()
        first = pl.multiple_of(i * block, block)
        rows = pl.ds(first, block)
        for r in range(block):
            w = jnp.concatenate([bias_w[...], gpair[first + r]], 0)
            rows_buf[r] = dot(w, pair_buf[first + r], NT)
        packed = jnp.ones((block, 128), F32)
        for h in range(heads):
            logit = lbase[h, rows, :] + scale * rows_buf[:, h, :]
            logit = jnp.where(valid, logit, F32(-1000000000.0))
            peak = jnp.max(logit, axis=1, keepdims=True)
            e = jnp.exp(logit - peak)
            d = dbase[h, rows, :] + rows_buf[:, PAD + h, :]
            lbase[h, rows, :] = e
            dbase[h, rows, :] = d
            packed = jnp.where(lane == h, peak, packed)
            packed = jnp.where(lane == PAD + h, jnp.sum(e, axis=1, keepdims=True), packed)
            packed = jnp.where(
                lane == 2 * PAD + h, jnp.sum(e * d, axis=1, keepdims=True), packed
            )
        stats[0, rows, :] = packed
        return carry

    lax.fori_loop(0, blocks, forward, 0)

    pl.semaphore_wait(barrier, nr_dev + nc_dev - 2)
    sent = []

    def stat_copy(s, peer):
        return remote(
            stats.at[0], stats.at[s], stat_send.at[s], stat_recv.at[s], {"col": peer}
        )

    for s, peer in enumerate(col_peers, 1):
        copy = stat_copy(s, peer)
        copy.start()
        sent.append(copy)
    for s, peer in enumerate(col_peers, 1):
        stat_copy(s, peer).wait_recv()
    factor, delta = merged(stats, stats[0])
    merge_buf[0] = factor
    merge_buf[1] = delta

    lane_of = lax.broadcasted_iota(jnp.int32, (n_rows, 128), 1)
    row_of = lax.broadcasted_iota(jnp.int32, (PAD, 128), 0)
    lane_small = lax.broadcasted_iota(jnp.int32, (PAD, 128), 1)
    small[...] = jnp.zeros_like(small)
    key_rows[...] = jnp.zeros_like(key_rows)
    query_rows[...] = jnp.zeros_like(query_rows)

    lead_heads, lead_lanes = lead

    def sums(shift, h, carry):
        mine = lane_of == h
        pick = lambda x: jnp.sum(jnp.where(mine, x, 0.0), axis=1, keepdims=True)
        att = lbase[h] * pick(merge_buf[0])
        dl = att * (dbase[h] - pick(merge_buf[1]))
        a0 = att.astype(BF16)
        d0, d1 = split2(dl)
        q = jnp.concatenate(split2(qcat[h]), 0)
        k = jnp.concatenate(split2(kcat[h]), 0)
        g = jnp.concatenate(split2(filled(gcat[h], PAD)), 0)
        v = jnp.concatenate(split2(filled(vcat[h], PAD)), 0)
        kk = dot(q, d0, NN) + dot(q, d1, NN)
        vv = dot(g, a0, NN)
        half = g.shape[0] // 2
        first = pl.multiple_of(h * (nq + nv) + shift, 8)
        key_rows[pl.ds(first, nq), :] = kk[:nq] + kk[nq:]
        key_rows[pl.ds(first + nq, nv), :] = vv[:nv] + vv[half : half + nv]
        qq = dot(k, d0, NT) + dot(k, d1, NT)
        qq = qq[:nq] + qq[nq:]
        oo = dot(v, a0, NT)
        first = pl.multiple_of(h * (nq + nv - vwidth), 8)
        query_rows[pl.ds(first, nq), :] = qq
        query_rows[pl.ds(first + nq, nv - vwidth), :] = (
            oo[vwidth:nv] + oo[half + vwidth : half + nv]
        )
        raw = qraw[h]
        span = qsize - vwidth
        part = raw[span : span + 1] * qq[qsize + 1 : qsize + 2] + qq[qsize : qsize + 1]
        part = part - 2.0 * jnp.sum(raw[:span] * qq[vwidth:qsize], axis=0, keepdims=True)
        part = jnp.sum(part, axis=1, keepdims=True)
        small[...] = small[...] + jnp.where(
            (row_of == heads) & (lane_small == h), part, 0.0
        )
        return carry

    share = cols // nr_dev
    lane_count = key_t.shape[2]
    bits = list(range(nr_dev.bit_length() - 1))
    swapped = bits[:1] + bits[1:3][::-1] + bits[3:]
    last = len(bits) - 1
    lane_parts = [pl.ds(0, lead_lanes), pl.ds(lead_lanes, lane_count - lead_lanes)]
    if len(slots) == 4:
        cut = share // 2
        halves = [(pl.ds(0, cut), bits), (pl.ds(cut, share - cut), swapped)]
        plans = [[(half, order) for half, order in halves]] * 2
    else:
        plans = [[(slice(None), bits)], [(slice(None), swapped)]]
    groups, count = [], 0
    for lanes_of, plan in zip(lane_parts, plans):
        group = []
        for half, order in plan:
            part = (half, lanes_of)
            group.append(
                Scatter(
                    me, key_t, part, order, slots[count], key_send.at[count], key_recv.at[count]
                )
            )
            count += 1
        groups.append(group)

    def begin(group, phase):
        for stream in groups[group]:
            if phase < last:
                stream.start(phase)

    def advance(group, phase):
        for stream in groups[group]:
            if phase < last:
                stream.finish(phase)
            if phase + 1 < last:
                stream.start(phase + 1)

    def upright_keys(first, end):
        for t in range(first // 128, end // 128):
            part = slice(128 * t, 128 * t + 128)
            key_t[:, :, part] = key_rows[part, :].T.reshape(nr_dev, share, 128)

    lax.fori_loop(0, lead_heads, functools.partial(sums, 0), 0)
    upright_keys(0, lead_lanes)
    begin(0, 0)
    shift = lead_lanes - lead_heads * (nq + nv)
    lax.fori_loop(lead_heads, heads, functools.partial(sums, shift), 0)
    upright_keys(lead_lanes, lane_count)
    advance(0, 0)
    begin(1, 0)
    qshare = n_rows // nc_dev
    for t in range(query_t.shape[2] // 128):
        part = slice(128 * t, 128 * t + 128)
        query_t[:, :, part] = query_rows[part, :].T.reshape(nc_dev, qshare, 128)

    def q_copy(s, peer):
        return remote(
            query_t.at[peer], qslots.at[s], q_send.at[s], q_recv.at[s], {"col": peer}
        )

    for s, peer in enumerate(col_peers):
        copy = q_copy(s, peer)
        copy.start()
        sent.append(copy)
    rows_buf[...] = jnp.zeros_like(rows_buf)

    depth = a_out.shape[1]

    def a_copy(i):
        rows = pl.ds(pl.multiple_of(i * block, block), block)
        return pltpu.make_async_copy(
            pair_buf.at[rows, pl.ds(0, depth), :], a_out.at[rows], a_sem.at[i]
        )

    def weights(i, carry):
        first = pl.multiple_of(i * block, block)
        rows = pl.ds(first, block)
        factor = merge_buf[0, rows, :]
        delta = merge_buf[1, rows, :]
        for h in range(heads):
            att = lbase[h, rows, :] * factor[:, h : h + 1]
            rows_buf[:, h, :] = att * (dbase[h, rows, :] - delta[:, h : h + 1])
            rows_buf[:, PAD + h, :] = att
        acc = small[...]
        for r in range(block):
            a = rows_buf[r].astype(BF16)
            acc = acc + scale * dot(a[:PAD], pair_buf[first + r], NN)
            for c in range(cols // 128):
                pair_buf[first + r, 2 * PAD * c : 2 * PAD * c + 2 * PAD, :] = a[
                    :, 128 * c : 128 * c + 128
                ]
        small[...] = acc

        @pl.when(i > 0)
        def _():
            a_copy(i - 1).start()

        return carry

    early, middle = blocks // 4, (5 * blocks) // 8
    lax.fori_loop(0, early, weights, 0)
    advance(1, 0)
    lax.fori_loop(early, middle, weights, 0)
    advance(0, 1)
    lax.fori_loop(middle, blocks, weights, 0)
    a_copy(blocks - 1).start()

    def col_copy(s, peer):
        return remote(
            small, small_col.at[s], col_send.at[s], col_recv.at[s], {"col": peer}
        )

    for s, peer in enumerate(col_peers):
        copy = col_copy(s, peer)
        copy.start()
        sent.append(copy)
    total = query_t[mc]
    for s, peer in enumerate(col_peers):
        q_copy(s, peer).wait_recv()
        total = total + qslots[s]
    query_t[mc] = total

    total = small[...]
    for s, peer in enumerate(col_peers):
        col_copy(s, peer).wait_recv()
        total = total + small_col[s]
    small_row[0] = total

    def row_copy(s, peer):
        return remote(
            small_row.at[0], small_row.at[s], row_send.at[s], row_recv.at[s], {"row": peer}
        )

    for s, peer in enumerate(row_peers, 1):
        copy = row_copy(s, peer)
        copy.start()
        sent.append(copy)
    advance(1, 1)
    for phase in range(2, last):
        advance(0, phase)
        advance(1, phase)
    leaving = [
        pltpu.make_async_copy(key_t.at[me], key_out, in_sem.at[0]),
        pltpu.make_async_copy(key_t.at[flip(me, last)], key_away, in_sem.at[1]),
        pltpu.make_async_copy(query_t.at[mc], query_out, in_sem.at[2]),
    ]
    total = small_row[0]
    for s, peer in enumerate(row_peers, 1):
        row_copy(s, peer).wait_recv()
        total = total + small_row[s]
    small_out[...] = total
    for copy in leaving:
        copy.start()
    for copy in sent:
        copy.wait_send()
    for copy in leaving:
        copy.wait()
    for group in groups:
        for stream in group:
            stream.drain()

    def end_copy(i, carry):
        a_copy(i).wait()
        return carry

    lax.fori_loop(0, blocks, end_copy, 0)


def pair_kernel(block, scale, a_in, bias_in, gpair, pg_out):
    heads, channels = bias_in.shape
    w_hi, w_lo = split2(
        jnp.concatenate(
            [scale * bias_in[...].astype(F32), jnp.zeros((PAD - heads, channels), F32)], 0
        )
    )
    for r in range(block):
        step = 2 * PAD
        a = jnp.concatenate(
            [a_in[r, at : at + step, :] for at in range(0, a_in.shape[1], step)], 1
        )
        lhs = jnp.concatenate([a, a[:PAD]], 0)
        rhs = jnp.concatenate([w_hi, gpair[r], w_lo], 0)
        pg_out[r] = dot(lhs, rhs, TN).astype(BF16)


def own_lanes(load, start, size, total):
    if total == size:
        return load(slice(None))
    first = pl.multiple_of((start // 128) * 128, 128)
    tile = load(pl.ds(first, 128))
    return pltpu.roll(tile, lax.rem(128 - lax.rem(start, 128), 128), 1)[:, :size]


def upright(ref, rows):
    for t in range(rows.shape[0] // 128):
        part = slice(128 * t, 128 * t + 128)
        rows[part, :] = ref(part).T


def tail_kernel(
    shape, key_own, key_more, query_part, small, head_w, rot, shift, query_points, grad_points,
    key_points, value_points,
    query_grad, query_point_grad, query_frame, key_grad, value_grad, key_point_grad,
    value_point_grad, key_frame, weight_total, head_grad,
    krows, qrows, dpoint, dvalue, wide,
):
    heads, scale, inner, point_factor, nq, nv, vwidth, qsize, lead = shape
    qpoints, vpoints = (qsize - vwidth) // 3, (nv - vwidth) // 3
    me = lax.axis_index("row")
    mc = lax.axis_index("col")
    coef = point_coef(head_w, point_factor)
    weight_total[...] = small[:heads, :]
    x = head_w[...]
    grads = small[heads : heads + 1, :heads]
    slope = -point_factor
    head_grad[...] = grads * slope / (1.0 + jnp.exp(-x))

    def flat(source, out):
        rows = source.shape[0]
        wide[0:rows, 0 : source.shape[1]] = source
        for t in range(wide.shape[0] // 128):
            piece = wide[128 * t : 128 * t + 128, :].T
            end = min(128, rows - 128 * t)
            if end > 0:
                out(slice(128 * t, 128 * t + end), piece[: source.shape[1], :end])

    wide[...] = jnp.zeros_like(wide)

    def put(ref):
        def store(lanes, value):
            ref[:, lanes] = value

        return store

    share = query_part.shape[0]
    upright(lambda part: query_part[:, part], qrows)
    start = mc * share
    base = me * (share * lax.axis_size("col")) + start
    total = rot.shape[2]
    turns = [
        [own_lanes(lambda s: rot[i, j : j + 1, s], base, share, total) for j in range(3)]
        for i in range(3)
    ]
    shifts = [own_lanes(lambda s: shift[i : i + 1, s], base, share, total) for i in range(3)]
    local = [
        own_lanes(lambda s: query_points[y, :, s], start, share, query_points.shape[2])
        for y in range(3)
    ]
    cotan = [
        own_lanes(lambda s: grad_points[y, :, s], start, share, grad_points.shape[2])
        for y in range(3)
    ]
    nr = nq + nv - vwidth
    flat(
        (scale * inner)
        * jnp.concatenate([qrows[nr * h : nr * h + vwidth] for h in range(heads)], 0),
        put(query_grad),
    )
    spin = lambda i, v: turns[i][0] * v[0] + turns[i][1] * v[1] + turns[i][2] * v[2]
    for i in range(3):
        qg = spin(i, local) + shifts[i]
        for h in range(heads):
            points = slice(qpoints * h, qpoints * h + qpoints)
            at = nr * h + vwidth + qpoints * i
            sums = qrows[nr * h + qsize + 1 : nr * h + qsize + 2]
            dpoint[i, points] = (-2.0 * pick_lane(coef, h)) * (
                qg[points] * sums - qrows[at : at + qpoints]
            )
            at = nr * h + nq + vpoints * i
            dvalue[i, vpoints * h : vpoints * h + vpoints] = qrows[at : at + vpoints]
    down = lambda v: jnp.sum(v, axis=0, keepdims=True)
    for y in range(3):
        query_point_grad[y] = (
            turns[0][y] * dpoint[0] + turns[1][y] * dpoint[1] + turns[2][y] * dpoint[2]
        )
    for i in range(3):
        away = dvalue[i] - shifts[i]
        for y in range(3):
            query_frame[i, y : y + 1] = down(dpoint[i] * local[y]) + down(away * cotan[y])
        query_frame[i, 3:4] = down(dpoint[i]) - down(spin(i, cotan))

    share = key_own.shape[0]
    upright(lambda part: key_own[:, part] + key_more[:, part], krows)
    start = me * share
    base = mc * (share * lax.axis_size("row")) + start
    turns = [
        [own_lanes(lambda s: rot[i, j : j + 1, s], base, share, total) for j in range(3)]
        for i in range(3)
    ]
    shifts = [own_lanes(lambda s: shift[i : i + 1, s], base, share, total) for i in range(3)]
    local = [
        own_lanes(lambda s: key_points[y, :, s], start, share, key_points.shape[2])
        for y in range(3)
    ]
    values = [
        own_lanes(lambda s: value_points[y, :, s], start, share, value_points.shape[2])
        for y in range(3)
    ]
    nk = nq + nv
    starts = [nk * h if h < lead[0] else lead[1] + nk * (h - lead[0]) for h in range(heads)]
    flat(jnp.concatenate([krows[at : at + vwidth] for at in starts], 0), put(key_grad))
    flat(
        jnp.concatenate([krows[at + nq : at + nq + vwidth] for at in starts], 0),
        put(value_grad),
    )
    for i in range(3):
        kg = spin(i, local) + shifts[i]
        for h in range(heads):
            points = slice(qpoints * h, qpoints * h + qpoints)
            at = starts[h] + vwidth + qpoints * i
            sums = krows[starts[h] + qsize : starts[h] + qsize + 1]
            dpoint[i, points] = krows[at : at + qpoints] + 2.0 * kg[points] * sums
            at = starts[h] + nq + vwidth + vpoints * i
            dvalue[i, vpoints * h : vpoints * h + vpoints] = krows[at : at + vpoints]
    for y in range(3):
        key_point_grad[y] = (
            turns[0][y] * dpoint[0] + turns[1][y] * dpoint[1] + turns[2][y] * dpoint[2]
        )
        flat(
            turns[0][y] * dvalue[0] + turns[1][y] * dvalue[1] + turns[2][y] * dvalue[2],
            put(value_point_grad.at[y]),
        )
    for i in range(3):
        for y in range(3):
            key_frame[i, y : y + 1] = down(dpoint[i] * local[y]) + down(dvalue[i] * values[y])
        key_frame[i, 3:4] = down(dpoint[i]) + down(dvalue[i])


def pad_rows(x, rows):
    return jnp.pad(x, ((0, 0), (0, rows - x.shape[1]), (0, 0)))


def per_device(
    pair_rep, bias_weight, head_weight, queries, key_vectors, values, query_points, key_points,
    value_points, rotations, translations, residue_count, grad_output, grad_points, grad_pair,
):
    channels, heads = bias_weight.shape
    width = queries.shape[0] // heads
    qpoints = query_points.shape[1] // heads
    vpoints = value_points.shape[1] // heads
    n_rows = queries.shape[1]
    n_cols = key_vectors.shape[1]
    logit_scale = math.sqrt(1.0 / 3.0)
    point_scale = math.sqrt(2.0 / (9.0 * qpoints))
    inner_scale = 1.0 / math.sqrt(width)
    point_factor = 0.5 * logit_scale * point_scale
    qsize = width + 3 * qpoints
    nq = -(-(qsize + 2) // 16) * 16
    nv = width + 3 * vpoints
    bias_t = bias_weight.T
    gpair = pad_rows(grad_pair, PAD)
    head_row = head_weight.reshape(1, heads)

    block = 8
    depth = n_cols // 128 * 2 * PAD
    rows_dev = lax.axis_size("row")
    cols_dev = lax.axis_size("col")
    nk = nq + nv
    nr = nq + nv - width
    fit = lambda n: -(-n * nk // 128) * 128
    lead_heads = min(range(heads // 2, heads), key=lambda n: fit(n) + fit(heads - n))
    lead = (lead_heads, fit(lead_heads))
    key_lanes = fit(lead_heads) + fit(heads - lead_heads)
    query_lanes = -(-heads * nr // 128) * 128
    kshare = n_cols // rows_dev
    qshare = n_rows // cols_dev
    slot_count = max(rows_dev - 2, 1)
    if kshare % 16 == 0:
        slot_shapes = [(slot_count, kshare // 2, lead[1])] * 2
        slot_shapes += [(slot_count, kshare // 2, key_lanes - lead[1])] * 2
    else:
        slot_shapes = [(slot_count, kshare, c) for c in (lead[1], key_lanes - lead[1])]
    rot_rows, shift_rows = rotations, translations
    if n_rows % 128:
        row_start = lax.axis_index("row") * n_rows
        rot_rows = lax.dynamic_slice_in_dim(rotations, row_start, n_rows, 2)
        shift_rows = lax.dynamic_slice_in_dim(translations, row_start, n_rows, 1)
    vmem = pl.BlockSpec(memory_space=pltpu.VMEM)
    anywhere = pl.BlockSpec(memory_space=pl.ANY)
    sems = lambda count: pltpu.SemaphoreType.DMA((max(count, 1),))
    a_all, key_own, key_away, query_part, small = pl.pallas_call(
        functools.partial(
            main_kernel,
            (
                heads, block, logit_scale, inner_scale, point_factor, rows_dev, cols_dev,
                nq, nv, width, qsize, lead,
            ),
        ),
        in_specs=[pl.BlockSpec(memory_space=pltpu.SMEM), anywhere] + [vmem] * 11 + [anywhere] * 4,
        out_specs=[anywhere] * 4 + [vmem],
        out_shape=[
            jax.ShapeDtypeStruct((n_rows, depth, 128), BF16),
            jax.ShapeDtypeStruct((kshare, key_lanes), F32),
            jax.ShapeDtypeStruct((kshare, key_lanes), F32),
            jax.ShapeDtypeStruct((qshare, query_lanes), F32),
            jax.ShapeDtypeStruct((PAD, channels), F32),
        ],
        scratch_shapes=[
            pltpu.VMEM((n_rows, n_cols, channels), BF16),
            pltpu.VMEM((heads, n_rows, n_cols), F32),
            pltpu.VMEM((heads, n_rows, n_cols), F32),
            pltpu.VMEM((block, 2 * PAD, n_cols), F32),
            pltpu.VMEM((cols_dev, n_rows, 128), F32),
            pltpu.VMEM((2, n_rows, 128), F32),
            pltpu.VMEM((key_lanes, n_cols), F32),
            pltpu.VMEM((rows_dev, kshare, key_lanes), F32),
            [pltpu.VMEM(dims, F32) for dims in slot_shapes],
            pltpu.VMEM((query_lanes, n_rows), F32),
            pltpu.VMEM((cols_dev, qshare, query_lanes), F32),
            pltpu.VMEM((max(cols_dev - 1, 1), qshare, query_lanes), F32),
            pltpu.VMEM((PAD, channels), F32),
            pltpu.VMEM((max(cols_dev - 1, 1), PAD, channels), F32),
            pltpu.VMEM((rows_dev, PAD, channels), F32),
            pltpu.VMEM((PAD, channels), BF16),
            pltpu.VMEM((heads, nq, n_rows), F32),
            pltpu.VMEM((heads, nq, n_cols), F32),
            pltpu.VMEM((heads, nv, n_rows), F32),
            pltpu.VMEM((heads, nv, n_cols), F32),
            pltpu.VMEM((heads, PAD, n_rows), F32),
            sems(n_rows // block),
            sems(n_rows // block),
            sems(4),
            sems(cols_dev),
            sems(cols_dev),
            pltpu.SemaphoreType.DMA((len(slot_shapes), slot_count)),
            pltpu.SemaphoreType.DMA((len(slot_shapes), slot_count)),
            sems(cols_dev - 1),
            sems(cols_dev - 1),
            sems(cols_dev - 1),
            sems(cols_dev - 1),
            sems(rows_dev),
            sems(rows_dev),
        ],
        compiler_params=pltpu.CompilerParams(
            collective_id=0, has_side_effects=True, vmem_limit_bytes=VMEM_LIMIT
        ),
    )(
        residue_count, pair_rep, bias_t, gpair, head_row, queries, query_points, grad_output,
        grad_points, rot_rows, shift_rows, rotations, translations,
        key_vectors.reshape(heads, width, n_cols), values.reshape(heads, width, n_cols),
        key_points.reshape(-1, n_cols), value_points.reshape(-1, n_cols),
    )
    half = rows_dev // 2
    key_more = lax.ppermute(key_away, "row", [(i, (i + half) % rows_dev) for i in range(rows_dev)])

    out_block = 16
    pair_grad = pl.pallas_call(
        functools.partial(pair_kernel, out_block, logit_scale),
        grid=(n_rows // out_block,),
        in_specs=[
            pl.BlockSpec((out_block, depth, 128), lambda i: (i, 0, 0)),
            pl.BlockSpec((heads, channels), lambda i: (0, 0)),
            pl.BlockSpec((out_block, PAD, channels), lambda i: (i, 0, 0)),
        ],
        out_specs=pl.BlockSpec((out_block, n_cols, channels), lambda i: (i, 0, 0)),
        out_shape=jax.ShapeDtypeStruct(pair_rep.shape, BF16),
        compiler_params=pltpu.CompilerParams(dimension_semantics=("arbitrary",)),
        cost_estimate=pl.CostEstimate(
            flops=4 * n_rows * n_cols * channels * PAD,
            bytes_accessed=2 * n_rows * n_cols * (channels + 2 * PAD),
            transcendentals=0,
        ),
    )(a_all, bias_t, gpair)

    local_q, local_g = query_points, grad_points
    if n_rows % 128:
        start = lax.axis_index("col") * qshare
        local_q = lax.dynamic_slice_in_dim(query_points, start, qshare, 2)
        local_g = lax.dynamic_slice_in_dim(grad_points, start, qshare, 2)
    most = max(kshare, qshare, 128)
    f32 = lambda *dims: jax.ShapeDtypeStruct(dims, F32)
    (
        query_grad, query_point_grad, query_frame_grad, key_grad, value_grad, key_point_grad,
        value_point_grad, key_frame_grad, weight_total, head_weight_grad,
    ) = pl.pallas_call(
        functools.partial(
            tail_kernel,
            (heads, logit_scale, inner_scale, point_factor, nq, nv, width, qsize, lead),
        ),
        in_specs=[vmem] * 11,
        out_specs=[vmem] * 10,
        out_shape=[
            f32(qshare, heads * width),
            f32(3, heads * qpoints, qshare),
            f32(3, 4, qshare),
            f32(kshare, heads * width),
            f32(kshare, heads * width),
            f32(3, heads * qpoints, kshare),
            f32(3, kshare, heads * vpoints),
            f32(3, 4, kshare),
            f32(heads, channels),
            f32(1, heads),
        ],
        scratch_shapes=[
            pltpu.VMEM((key_lanes, kshare), F32),
            pltpu.VMEM((query_lanes, qshare), F32),
            pltpu.VMEM((3, heads * qpoints, kshare), F32),
            pltpu.VMEM((3, heads * vpoints, kshare), F32),
            pltpu.VMEM((-(-heads * width // 128) * 128, most), F32),
        ],
    )(
        key_own, key_more, query_part, small, head_row, rotations, translations, local_q,
        local_g, key_points, value_points,
    )
    query_grad, key_grad, value_grad = query_grad.T, key_grad.T, value_grad.T
    value_point_grad = value_point_grad.transpose(0, 2, 1)
    weight_total, head_weight_grad = weight_total.T, head_weight_grad.reshape(heads)
    return (
        pair_grad, query_grad, query_point_grad, query_frame_grad, key_grad, value_grad,
        key_point_grad, value_point_grad, key_frame_grad, weight_total, head_weight_grad,
    )


def solution(mesh):
    return jax.shard_map(
        per_device,
        mesh=mesh,
        in_specs=(
            P("row", "col", None),
            P(),
            P(),
            P(None, "row"),
            P(None, "col"),
            P(None, "col"),
            P(None, None, "row"),
            P(None, None, "col"),
            P(None, None, "col"),
            P(),
            P(),
            P(),
            P(None, "row"),
            P(None, None, "row"),
            P("row", None, None),
        ),
        out_specs=(
            P("row", "col", None),
            P(None, ("row", "col")),
            P(None, None, ("row", "col")),
            P(None, None, ("row", "col")),
            P(None, ("col", "row")),
            P(None, ("col", "row")),
            P(None, None, ("col", "row")),
            P(None, None, ("col", "row")),
            P(None, None, ("col", "row")),
            P(),
            P(),
        ),
        check_vma=False,
    )
```
